128 devices in a mesh: dep: 4 (over z), col: 4 (over y), row: 8 (over x, core).
Axes of the slice: x: 4, y: 4, z: 4, core: 2. Of those that a mesh axis runs over, the one named last changes fastest.
Arguments:
- x_tok: bfloat16 [8192, 4096], P(('dep', 'row'), 'col')
- w_up: bfloat16 [4096, 16384], P('row', 'col')
- w_down: bfloat16 [16384, 4096], P('row', 'col')
- grad_out: bfloat16 [8192, 4096], P(('dep', 'row'), 'col')
Outputs:
- output 1: bfloat16 [8192, 4096], P(('dep', 'row'), 'col')
- output 2: bfloat16 [8192, 4096], P(('dep', 'row'), 'col')
- output 3: float32 [4096, 16384], P(('row', 'dep'), 'col')
- output 4: float32 [16384, 4096], P(('row', 'dep'), 'col')
All inputs are finite; a program needn't handle non-finite values.
Results may differ from the reference program's by a relative error of at most 0.001.
Values are sent between devices in bfloat16 or wider.
A program may use at most 1 GiB of HBM per device.

```python
import math
import jax
import jax.numpy as jnp
from jax import lax

HIDDEN = 4096
FFN_DIM = 16384
TOKENS = 8192

BLOCK_ROWS = math.gcd(TOKENS, 2048)
NUM_BLOCKS = TOKENS // BLOCK_ROWS
GELU_COEF = 0.7978845608028654
CUBIC_COEF = 0.044715


def gelu_fwd(pre_act):
    inner = GELU_COEF * (pre_act + CUBIC_COEF * pre_act * pre_act * pre_act)
    return 0.5 * pre_act * (1.0 + jnp.tanh(inner))


def gelu_slope(pre_act):
    inner = GELU_COEF * (pre_act + CUBIC_COEF * pre_act * pre_act * pre_act)
    tanh_val = jnp.tanh(inner)
    return 0.5 * (1.0 + tanh_val) + 0.5 * pre_act * (1.0 - tanh_val * tanh_val) * GELU_COEF * (1.0 + 3.0 * CUBIC_COEF * pre_act * pre_act)


def setup_inputs(seed: int = 0) -> dict:
    root_key = jax.random.key(seed)
    key_x, key_up, key_down, key_g = jax.random.split(root_key, 4)
    x_tok = jax.random.normal(key_x, (TOKENS, HIDDEN), jnp.float32).astype(jnp.bfloat16)
    w_up = (jax.random.normal(key_up, (HIDDEN, FFN_DIM), jnp.float32) * HIDDEN ** -0.5).astype(jnp.bfloat16)
    w_down = (jax.random.normal(key_down, (FFN_DIM, HIDDEN), jnp.float32) * FFN_DIM ** -0.5).astype(jnp.bfloat16)
    grad_out = jax.random.normal(key_g, (TOKENS, HIDDEN), jnp.float32).astype(jnp.bfloat16)
    return {"x_tok": x_tok, "w_up": w_up, "w_down": w_down, "grad_out": grad_out}


def reference(x_tok, w_up, w_down, grad_out):
    x_blocks = x_tok.reshape(NUM_BLOCKS, BLOCK_ROWS, HIDDEN)
    g_blocks = grad_out.reshape(NUM_BLOCKS, BLOCK_ROWS, HIDDEN)

    def block_step(acc_pair, block_in):
        dw_up_acc, dw_down_acc = acc_pair
        x_blk, g_blk = block_in
        pre_act = jnp.dot(x_blk, w_up, preferred_element_type=jnp.float32)
        hidden_act = gelu_fwd(pre_act).astype(jnp.bfloat16)
        y_blk = jnp.dot(hidden_act, w_down, preferred_element_type=jnp.float32).astype(jnp.bfloat16)
        d_act = jnp.dot(g_blk, w_down.T, preferred_element_type=jnp.float32)
        d_pre = (d_act * gelu_slope(pre_act)).astype(jnp.bfloat16)
        dx_blk = jnp.dot(d_pre, w_up.T, preferred_element_type=jnp.float32).astype(jnp.bfloat16)
        dw_up_acc = dw_up_acc + jnp.dot(x_blk.T, d_pre, preferred_element_type=jnp.float32)
        dw_down_acc = dw_down_acc + jnp.dot(hidden_act.T, g_blk, preferred_element_type=jnp.float32)
        return (dw_up_acc, dw_down_acc), (y_blk, dx_blk)

    init_acc = (jnp.zeros((HIDDEN, FFN_DIM), jnp.float32), jnp.zeros((FFN_DIM, HIDDEN), jnp.float32))
    (dw_up, dw_down), (y_blocks, dx_blocks) = lax.scan(block_step, init_acc, (x_blocks, g_blocks))
    return y_blocks.reshape(TOKENS, HIDDEN), dx_blocks.reshape(TOKENS, HIDDEN), dw_up, dw_down
```

```python
import jax
import jax.numpy as jnp
from jax import lax
from jax.experimental import pallas as pl
from jax.experimental.pallas import tpu as pltpu
from jax.sharding import PartitionSpec as P

GELU_COEF = 0.7978845608028654
CUBIC_COEF = 0.044715
NX = 4
NY = 4
NZ = 4


def gelu_fwd(pre_act):
    inner = GELU_COEF * (pre_act + CUBIC_COEF * pre_act * pre_act * pre_act)
    return 0.5 * pre_act * (1.0 + jnp.tanh(inner))


def gelu_slope(pre_act):
    inner = GELU_COEF * (pre_act + CUBIC_COEF * pre_act * pre_act * pre_act)
    tanh_val = jnp.tanh(inner)
    return 0.5 * (1.0 + tanh_val) + 0.5 * pre_act * (1.0 - tanh_val * tanh_val) * GELU_COEF * (1.0 + 3.0 * CUBIC_COEF * pre_act * pre_act)


def rot(v, d, n):
    return lax.rem(v + (d % n), n)


class Net:
    def __init__(self, send_sem, recv_sem):
        self.send_sem, self.recv_sem = send_sem, recv_sem
        self.used = 0
        self.sent = []
        self.z = lax.axis_index("dep")
        self.y = lax.axis_index("col")
        row = lax.axis_index("row")
        self.row = row
        self.x = lax.div(row, 2)
        self.k = lax.rem(row, 2)

    def slots(self, n):
        base = self.used
        self.used += n
        return base

    def make(self, src, dst, where, send_slot, recv_slot):
        return pltpu.make_async_remote_copy(
            src_ref=src, dst_ref=dst, send_sem=self.send_sem.at[send_slot], recv_sem=self.recv_sem.at[recv_slot],
            device_id=where, device_id_type=pl.DeviceIdType.MESH)

    def send(self, src, dst, where):
        slot = self.slots(1)
        copy = self.make(src, dst, where, slot, slot)
        copy.start()
        self.sent.append(copy)
        return copy

    def finish(self):
        for copy in self.sent:
            copy.wait_send()

    def at_x(self, d):
        return {"row": 2 * rot(self.x, d, NX) + self.k}

    def at_y(self, d):
        return {"col": rot(self.y, d, NY)}

    def at_z(self, d):
        return {"dep": rot(self.z, d, NZ)}

    def partner(self):
        return {"row": 2 * self.x + 1 - self.k}


def ring(net, place, n, up, down, own, view, arrived):
    e_lo = net.send(own(0), view(place, 0), up)
    w_hi = net.send(own(1), view(place, 1), down)
    e_hi = net.send(own(1), view(place, 1), up)
    w_lo = net.send(own(0), view(place, 0), down)
    west, east, far = rot(place, -1, n), rot(place, 1, n), rot(place, 2, n)
    yield
    e_lo.wait_recv()
    on_up = net.send(view(west, 0), view(west, 0), up)
    arrived(west, 0)
    yield
    w_hi.wait_recv()
    on_down = net.send(view(east, 1), view(east, 1), down)
    arrived(east, 1)
    yield
    e_hi.wait_recv()
    arrived(west, 1)
    w_lo.wait_recv()
    arrived(east, 0)
    yield
    on_up.wait_recv()
    arrived(far, 0)
    on_down.wait_recv()
    arrived(far, 1)


def to_z(net, view, got):
    def arrived(i, half):
        got.append(net.send(view(i, half), view(i, half), net.at_z(1 if half == 0 else -1)))
    return arrived


def gather_w1(net, w1, w1f, buf, sem):
    rows, cols = w1.shape[0], w1f.shape[1]
    half = rows // 2
    parity = lax.rem(net.z, 2)
    mine = pl.ds(pl.multiple_of(net.k * cols, cols), cols)
    other = pl.ds(pl.multiple_of((1 - net.k) * cols, cols), cols)
    own_rows = pl.ds(pl.multiple_of(net.row * rows, rows), rows)
    load = pltpu.make_async_copy(w1.at[:, mine], buf, sem.at[0])
    load.start()
    swap = net.send(w1.at[:, other], w1f.at[own_rows, :], net.partner())
    load.wait()
    store = pltpu.make_async_copy(buf, w1f.at[own_rows, :], sem.at[0])
    store.start()
    yield
    swap.wait_recv()
    store.wait()

    def view(i, h):
        return w1f.at[pl.ds(pl.multiple_of((2 * i + parity) * rows + h * half, half), half), :]

    got = []
    yield from ring(net, net.x, NX, net.at_x(1), net.at_x(-1), lambda h: view(net.x, h), view, to_z(net, view, got))
    yield
    for copy in got:
        copy.wait_recv()


def gather_tokens(net, src, dst, buf, sem):
    rows, cols = src.shape
    rs = pl.ds(pl.multiple_of(net.k * rows, rows), rows)

    def view(j):
        return dst.at[rs, pl.ds(pl.multiple_of(j * cols, cols), cols)]

    load = pltpu.make_async_copy(src, buf, sem)
    load.start()
    copies = [net.send(src, view(net.y), net.at_y(d)) for d in (1, 3, 2)]
    passed = [net.send(src, view(net.y), net.partner())]
    load.wait()
    store = pltpu.make_async_copy(buf, view(net.y), sem)
    store.start()
    yield
    for d, copy in zip((1, 3, 2), copies):
        copy.wait_recv()
        piece = view(rot(net.y, -d, NY))
        passed.append(net.send(piece, piece, net.partner()))
        yield
    store.wait()
    for copy in passed:
        copy.wait_recv()


def scatter(net, pieces, slot_of, dev_of, self_piece, is_self, here, arrivals, sender, buf, sem):
    send_base, recv_base = net.slots(4), 0
    load = pltpu.make_async_copy(self_piece, buf, sem)
    load.start()
    copies = []
    for s in range(4):
        copy = net.make(pieces(s), slot_of(s), dev_of(s), send_base + s, send_base + sender)
        stays = is_self(s)
        copies.append((copy, stays))

        @pl.when(jnp.logical_not(stays))
        def _():
            copy.start()

    load.wait()

    @pl.when(here)
    def _():
        pltpu.make_async_copy(buf, arrivals(sender), net.recv_sem.at[send_base + sender]).start()

    yield
    for i in range(4):
        net.make(buf, arrivals(i), dev_of(0), send_base, send_base + i).wait_recv()
    yield
    for copy, stays in copies:
        @pl.when(jnp.logical_not(stays))
        def _():
            copy.wait_send()


def scatter_w2(net, w2, w2s, buf, sem):
    rows, cols = w2.shape
    part = rows // 8
    parity = lax.rem(net.z, 2)

    def piece(s):
        return w2.at[pl.ds(pl.multiple_of(parity * 4 * part + s * part, part), part), :]

    def slot(j):
        return w2s.at[:, pl.ds(pl.multiple_of(j * cols, cols), cols)]

    yield from scatter(
        net, piece, lambda s: slot(net.y), lambda s: {"col": net.x, "row": 2 * s + net.k}, piece(net.x),
        lambda s: jnp.logical_and(net.x == s, net.y == net.x), net.x == net.y, slot, net.y, buf, sem)


def gather_w2(net, w2s, w2f, buf, sem):
    rows = w2s.shape[0]
    half = rows // 2
    parity = lax.rem(net.z, 2)
    load = pltpu.make_async_copy(w2s, buf, sem)
    load.start()

    def view(i, h):
        return w2f.at[pl.ds(pl.multiple_of(parity * 4 * rows + i * rows + h * half, half), half), :]

    got = []
    arrived = to_z(net, view, got)
    gather = ring(net, net.x, NX, net.at_x(1), net.at_x(-1), lambda h: w2s.at[pl.ds(h * half, half), :], view, arrived)
    next(gather)
    got.append(net.send(w2s.at[pl.ds(0, half), :], view(net.x, 0), net.at_z(1)))
    got.append(net.send(w2s.at[pl.ds(half, half), :], view(net.x, 1), net.at_z(-1)))
    load.wait()
    store = pltpu.make_async_copy(buf, w2f.at[pl.ds(pl.multiple_of(parity * 4 * rows + net.x * rows, rows), rows), :], sem)
    store.start()
    yield
    yield from gather
    yield
    for copy in got:
        copy.wait_recv()
    store.wait()


def move_act(net, act, act_l, buf, sem):
    part = act_l.shape[2]
    yield from scatter(
        net, lambda s: act.at[pl.ds(s * part, part), :], lambda s: act_l.at[net.x, s],
        lambda s: {"row": 2 * net.y + net.k, "col": s}, act.at[pl.ds(pl.multiple_of(net.y * part, part), part), :],
        lambda s: jnp.logical_and(net.y == s, net.x == net.y), net.x == net.y,
        lambda i: act_l.at[i, net.y], net.x, buf, sem)

    def view(j, h):
        return act_l.at[pl.ds(2 * h, 2), j]

    yield from ring(net, net.y, NY, net.at_y(1), net.at_y(-1), lambda h: view(net.y, h), view, lambda i, h: None)


def layer_tokens(net, own, piece, dst, buf, sem):
    load = pltpu.make_async_copy(own, buf, sem)
    load.start()
    copies = [net.send(piece(d), dst.at[net.row], net.at_x(d)) for d in (1, 3, 2)]
    passed = [net.send(own, dst.at[net.row], net.partner())]
    load.wait()
    store = pltpu.make_async_copy(buf, dst.at[net.row], sem)
    store.start()
    yield
    for d, copy in zip((1, 3, 2), copies):
        copy.wait_recv()
        block = dst.at[2 * rot(net.x, -d, NX) + net.k]
        passed.append(net.send(block, block, net.partner()))
        yield
    store.wait()
    for copy in passed:
        copy.wait_recv()


def gather_dpre(net, d_pre, d_pre_l, buf, sem):
    half = d_pre.shape[0] // 2
    load = pltpu.make_async_copy(d_pre, buf, sem)
    load.start()

    def view(i, h):
        return d_pre_l.at[i, pl.ds(h * half, half), :]

    gather = ring(net, net.x, NX, net.at_x(1), net.at_x(-1), lambda h: d_pre.at[pl.ds(h * half, half), :], view, lambda i, h: None)
    next(gather)
    load.wait()
    store = pltpu.make_async_copy(buf, d_pre_l.at[net.x], sem)
    store.start()
    yield
    yield from gather
    store.wait()


def exchange_sums(net, part, dst):
    cols = dst.shape[2]
    copies = []
    for d in (1, 3, 2):
        src = part.at[:, pl.ds(pl.multiple_of(rot(net.y, d, NY) * cols, cols), cols)]
        copies.append(net.send(src, dst.at[d - 1], net.at_y(d)))
    yield
    for copy in copies:
        copy.wait_recv()


def run(flows):
    flows = list(flows)
    while flows:
        flows = [f for f in flows if next(f, flows) is not flows]


def first_gather(w1, w2, x, g, w1f, w2s, xf, gf, b1, b2, bx, bg, lsem, ssem, rsem):
    net = Net(ssem, rsem)
    one = gather_w1(net, w1, w1f, b1, lsem)
    next(one)
    tokens = [gather_tokens(net, x, xf, bx, lsem.at[1]), gather_tokens(net, g, gf, bg, lsem.at[2])]
    for f in tokens:
        next(f)
    next(one)
    next(one)
    next(one)
    two = scatter_w2(net, w2, w2s, b2, lsem.at[3])
    run([one] + tokens + [two])
    net.finish()


def second_gather(w2s, act, g, w2f, act_l, g_l, b2, ba, bg, lsem, ssem, rsem):
    net = Net(ssem, rsem)
    acts = move_act(net, act, act_l, ba, lsem.at[1])
    next(acts)
    two = gather_w2(net, w2s, w2f, b2, lsem.at[0])
    next(two)
    toks = layer_tokens(net, g, lambda d: g, g_l, bg, lsem.at[2])
    run([two, acts, toks])
    net.finish()


def third_gather(d_pre, xf, ys, dxs, d_pre_l, x_l, yb, dxb, bd, bx, lsem, ssem, rsem):
    net = Net(ssem, rsem)
    rows, cols = bx.shape
    dp = gather_dpre(net, d_pre, d_pre_l, bd, lsem.at[0])
    next(dp)

    def piece(d):
        c = rot(net.x, d, NX)
        return xf.at[pl.ds(pl.multiple_of(net.k * rows, rows), rows), pl.ds(pl.multiple_of(c * cols, cols), cols)]

    toks = layer_tokens(net, piece(0), piece, x_l, bx, lsem.at[1])
    run([exchange_sums(net, ys, yb), exchange_sums(net, dxs, dxb), dp, toks])
    net.finish()


def comm(body, outs, bufs, n_local, n_remote, *args):
    hbm = pl.BlockSpec(memory_space=pltpu.HBM)
    return pl.pallas_call(
        body,
        out_shape=[jax.ShapeDtypeStruct(s, d) for s, d in outs],
        in_specs=[hbm] * len(args),
        out_specs=[hbm] * len(outs),
        scratch_shapes=[pltpu.VMEM(s, d) for s, d in bufs] + [
            pltpu.SemaphoreType.DMA((n_local,)), pltpu.SemaphoreType.DMA((n_remote,)), pltpu.SemaphoreType.DMA((n_remote,))],
        compiler_params=pltpu.CompilerParams(has_side_effects=True),
        cost_estimate=pl.CostEstimate(flops=80_000_000_000, bytes_accessed=64 << 20, transcendentals=0),
    )(*args)


def solution(mesh):
    act_spec = P(("dep", "row"), "col")
    wgt_spec = P("row", "col")
    grad_spec = P(("row", "dep"), "col")
    bf16, f32 = jnp.bfloat16, jnp.float32
    swap = [(r, r ^ 1) for r in range(2 * NX)]

    def dot(a, b, dims):
        return lax.dot_general(a, b, (dims, ((), ())), preferred_element_type=f32)

    def local_block(x_loc, w_up, w_down, g_loc):
        tb, hb = x_loc.shape
        hr, fb = w_up.shape
        fk = fb // 2
        hid = NY * hb
        tok = 2 * tb
        k = lax.rem(lax.axis_index("row"), 2)
        y = lax.axis_index("col")

        w1f, w2s, xf, gf = comm(
            first_gather,
            [((2 * NX * hr, fk), bf16), ((fk // 8, hid), bf16), ((tok, hid), bf16), ((tok, hid), bf16)],
            [((hr, fk), bf16), ((fk // 8, hb), bf16), ((tb, hb), bf16), ((tb, hb), bf16)], 4, 32,
            w_up, w_down, x_loc, g_loc)
        pre_act = dot(xf, w1f, ((1,), (0,)))
        act = gelu_fwd(pre_act).astype(bf16)
        w2f, act_l, g_l = comm(
            second_gather,
            [((fk, hid), bf16), ((NX, 4, tok // 4, fk), bf16), ((2 * NX, tb, hb), bf16)],
            [((fk // 8, hid), bf16), ((tok // 4, fk), bf16), ((tb, hb), bf16)], 3, 40,
            w2s, act, g_loc)
        d_act = dot(gf, w2f, ((1,), (1,)))
        d_pre = (d_act * gelu_slope(pre_act)).astype(bf16)
        dw_down_part = dot(act_l.reshape(NX * tok, fk), g_l.reshape(NX * tok, hb), ((0,), (0,)))
        dw_down = lax.psum_scatter(dw_down_part, "dep", scatter_dimension=0, tiled=True)

        def core_sum(part):
            keep = lax.dynamic_slice_in_dim(part, k * tb, tb, 0)
            give = lax.dynamic_slice_in_dim(part, (1 - k) * tb, tb, 0)
            return keep + lax.ppermute(give, "row", swap)

        ys = core_sum(dot(act, w2f, ((1,), (0,))))
        dxs = core_sum(dot(d_pre, w1f, ((1,), (1,))))
        d_pre, dw_down_part = lax.optimization_barrier((d_pre, dw_down_part))
        d_pre_l, x_l, yb, dxb = comm(
            third_gather,
            [((NX, tok, fk), bf16), ((2 * NX, tb, hb), bf16), ((3, tb, hb), f32), ((3, tb, hb), f32)],
            [((tok, fk), bf16), ((tb, hb), bf16)], 2, 32,
            d_pre, xf, ys, dxs)

        def col_sum(own, others):
            return (lax.dynamic_slice_in_dim(own, y * hb, hb, 1) + others[0] + others[1] + others[2]).astype(bf16)

        d_pre_l = d_pre_l.reshape(NX * tok, fk)
        x_l = x_l.reshape(NX * tok, hb)
        sums = []
        for c in range(2):
            part = dot(x_l[:, c * hr:(c + 1) * hr], d_pre_l, ((0,), (0,)))
            sums.append(lax.psum_scatter(part, "dep", scatter_dimension=0, tiled=True))
        keep = jnp.where(k == 0, sums[0], sums[1])
        take = lax.ppermute(jnp.where(k == 0, sums[1], sums[0]), "row", swap)
        dw_up = jnp.concatenate([jnp.where(k == 0, keep, take), jnp.where(k == 0, take, keep)], axis=1)
        return col_sum(ys, yb), col_sum(dxs, dxb), dw_up, dw_down

    return jax.shard_map(local_block, mesh=mesh, in_specs=(act_spec, wgt_spec, wgt_spec, act_spec), out_specs=(act_spec, act_spec, grad_spec, grad_spec), check_vma=False)
```

```python
import jax
import jax.numpy as jnp
from jax import lax
from jax.experimental import pallas as pl
from jax.experimental.pallas import tpu as pltpu
from jax.sharding import PartitionSpec as P

GELU_COEF = 0.7978845608028654
CUBIC_COEF = 0.044715
NX = 4
NY = 4
NZ = 4


def gelu_fwd(pre_act):
    inner = GELU_COEF * (pre_act + CUBIC_COEF * pre_act * pre_act * pre_act)
    return 0.5 * pre_act * (1.0 + jnp.tanh(inner))


def gelu_slope(pre_act):
    inner = GELU_COEF * (pre_act + CUBIC_COEF * pre_act * pre_act * pre_act)
    tanh_val = jnp.tanh(inner)
    return 0.5 * (1.0 + tanh_val) + 0.5 * pre_act * (1.0 - tanh_val * tanh_val) * GELU_COEF * (1.0 + 3.0 * CUBIC_COEF * pre_act * pre_act)


def rot(v, d, n):
    return lax.rem(v + (d % n), n)


class Net:
    def __init__(self, send_sem, recv_sem):
        self.send_sem, self.recv_sem = send_sem, recv_sem
        self.used = 0
        self.sent = []
        self.z = lax.axis_index("dep")
        self.y = lax.axis_index("col")
        row = lax.axis_index("row")
        self.row = row
        self.x = lax.div(row, 2)
        self.k = lax.rem(row, 2)

    def slots(self, n):
        base = self.used
        self.used += n
        return base

    def make(self, src, dst, where, send_slot, recv_slot):
        return pltpu.make_async_remote_copy(
            src_ref=src, dst_ref=dst, send_sem=self.send_sem.at[send_slot], recv_sem=self.recv_sem.at[recv_slot],
            device_id=where, device_id_type=pl.DeviceIdType.MESH)

    def send(self, src, dst, where):
        slot = self.slots(1)
        copy = self.make(src, dst, where, slot, slot)
        copy.start()
        self.sent.append(copy)
        return copy

    def finish(self):
        for copy in self.sent:
            copy.wait_send()

    def at_x(self, d):
        return {"row": 2 * rot(self.x, d, NX) + self.k}

    def at_y(self, d):
        return {"col": rot(self.y, d, NY)}

    def at_z(self, d):
        return {"dep": rot(self.z, d, NZ)}

    def partner(self):
        return {"row": 2 * self.x + 1 - self.k}


def ring(net, place, n, up, down, own, view, arrived, pieces=2):
    west, east, far = rot(place, -1, n), rot(place, 1, n), rot(place, 2, n)
    ups, downs, relays = [], [], []
    for q in range(pieces):
        if q == pieces // 2:
            yield
        r = pieces - 1 - q
        ups.append(net.send(own(q), view(place, q), up))
        downs.append(net.send(own(r), view(place, r), down))
    for q in range(pieces):
        yield
        r = pieces - 1 - q
        ups[q].wait_recv()
        if q < pieces // 2:
            relays.append((q, net.send(view(west, q), view(west, q), up)))
        arrived(west, q)
        downs[q].wait_recv()
        if q < pieces // 2:
            relays.append((r, net.send(view(east, r), view(east, r), down)))
        arrived(east, r)
    for q, copy in relays:
        yield
        copy.wait_recv()
        arrived(far, q)


def exchange(net, place, n, up, down, piece, slot, tmp, arrived=lambda j: None):
    west, east, far = rot(place, -1, n), rot(place, 1, n), rot(place, 2, n)
    lo = net.send(piece(far, 0), tmp.at[0], up)
    hi = net.send(piece(far, 1), tmp.at[1], down)
    e = net.send(piece(east, None), slot(place, 0, None), up)
    w = net.send(piece(west, None), slot(place, 1, None), down)
    yield
    lo.wait_recv()
    lo = net.send(tmp.at[0], slot(west, 2, 0), up)
    hi.wait_recv()
    hi = net.send(tmp.at[1], slot(east, 2, 1), down)
    yield
    e.wait_recv()
    arrived(west)
    w.wait_recv()
    arrived(east)
    yield
    lo.wait_recv()
    hi.wait_recv()
    arrived(far)


def rows_of(base, size, h):
    return pl.ds(base, size) if h is None else pl.ds(base + h * (size // 2), size // 2)


def to_z(net, view, got, pieces):
    def arrived(i, q):
        got.append(net.send(view(i, q), view(i, q), net.at_z(1 if q < pieces // 2 else -1)))
    return arrived


def gather_w1(net, w1, w1f, buf, sem):
    rows, cols = w1.shape[0], w1f.shape[1]
    size = rows // 4
    parity = lax.rem(net.z, 2)
    mine = pl.ds(pl.multiple_of(net.k * cols, cols), cols)
    other = pl.ds(pl.multiple_of((1 - net.k) * cols, cols), cols)
    own_rows = pl.ds(pl.multiple_of(net.row * rows, rows), rows)
    load = pltpu.make_async_copy(w1.at[:, mine], buf, sem)
    load.start()
    swap = net.send(w1.at[:, other], w1f.at[own_rows, :], net.partner())
    yield
    load.wait()
    store = pltpu.make_async_copy(buf, w1f.at[own_rows, :], sem)
    store.start()
    swap.wait_recv()
    store.wait()

    def view(i, q):
        return w1f.at[pl.ds(pl.multiple_of((2 * i + parity) * rows + q * size, size), size), :]

    got = []
    yield from ring(net, net.x, NX, net.at_x(1), net.at_x(-1), lambda q: view(net.x, q), view, to_z(net, view, got, 4), 4)
    yield
    for copy in got:
        copy.wait_recv()


def gather_tokens(net, src, dst, buf, sem):
    rows, cols = src.shape
    base = pl.multiple_of(net.k * rows, rows)

    def view(j, h):
        return dst.at[rows_of(base, rows, h), pl.ds(pl.multiple_of(j * cols, cols), cols)]

    load = pltpu.make_async_copy(src, buf, sem)
    load.start()
    passed = [net.send(src, view(net.y, None), net.partner())]

    def arrived(j, h):
        passed.append(net.send(view(j, h), view(j, h), net.partner()))

    gather = ring(net, net.y, NY, net.at_y(1), net.at_y(-1), lambda h: src.at[rows_of(0, rows, h), :], view, arrived)
    next(gather)
    load.wait()
    store = pltpu.make_async_copy(buf, view(net.y, None), sem)
    store.start()
    yield from gather
    yield
    store.wait()
    for copy in passed:
        copy.wait_recv()


def move_w2(net, w2, w2s, mid, tx, ty, sem):
    rows, cols = w2.shape
    part = rows // 8
    base = pl.multiple_of(lax.rem(net.z, 2) * 4 * part, part)

    def piece(i, h):
        return w2.at[rows_of(pl.multiple_of(base + i * part, part), part, h), :]

    load = pltpu.make_async_copy(piece(net.x, None), mid.at[net.x], sem)
    load.start()
    yield from exchange(net, net.x, NX, net.at_x(1), net.at_x(-1), piece, lambda j, side, h: mid.at[j, rows_of(0, part, h), :], tx)
    load.wait()

    def slot(j, side, h):
        return w2s.at[rows_of(0, part, h), pl.ds(pl.multiple_of(j * cols, cols), cols)]

    store = pltpu.make_async_copy(mid.at[net.y], slot(net.y, 0, None), sem)
    store.start()
    yield from exchange(net, net.y, NY, net.at_y(1), net.at_y(-1), lambda i, h: mid.at[i, rows_of(0, part, h), :], slot, ty)
    store.wait()


def gather_w2(net, w2s, w2f, buf, sem):
    rows = w2s.shape[0]
    size = rows // 4
    base = lax.rem(net.z, 2) * 4 * rows
    load = pltpu.make_async_copy(w2s, buf, sem)
    load.start()

    def view(i, q):
        return w2f.at[pl.ds(pl.multiple_of(base + i * rows + q * size, size), size), :]

    def own(q):
        return w2s.at[pl.ds(q * size, size), :]

    got = []
    gather = ring(net, net.x, NX, net.at_x(1), net.at_x(-1), own, view, to_z(net, view, got, 4), 4)
    next(gather)
    for q in (0, 3, 1, 2):
        got.append(net.send(own(q), view(net.x, q), net.at_z(1 if q < 2 else -1)))
    load.wait()
    store = pltpu.make_async_copy(buf, w2f.at[pl.ds(pl.multiple_of(base + net.x * rows, rows), rows), :], sem)
    store.start()
    yield
    yield from gather
    yield
    for copy in got:
        copy.wait_recv()
    store.wait()


def move_act(net, act, act_l, mid, tx, ty, sem):
    part = act_l.shape[2]

    def piece(i, h):
        return act.at[rows_of(pl.multiple_of(i * part, part), part, h), :]

    load = pltpu.make_async_copy(piece(net.y, None), mid.at[net.y], sem)
    load.start()
    yield from exchange(net, net.y, NY, net.at_y(1), net.at_y(-1), piece, lambda j, side, h: mid.at[j, rows_of(0, part, h), :], ty)
    load.wait()
    store = pltpu.make_async_copy(mid.at[net.x], act_l.at[net.x, net.y], sem)
    store.start()
    yield from exchange(
        net, net.x, NX, net.at_x(1), net.at_x(-1), lambda i, h: mid.at[i, rows_of(0, part, h), :],
        lambda j, side, h: act_l.at[j, net.y, rows_of(0, part, h), :], tx)
    store.wait()

    def view(j, h):
        return act_l.at[pl.ds(2 * h, 2), j]

    yield from ring(net, net.y, NY, net.at_y(1), net.at_y(-1), lambda h: view(net.y, h), view, lambda i, h: None)


def layer_g(net, g, g_l, buf, sem):
    rows = g.shape[0]
    load = pltpu.make_async_copy(g, buf, sem)
    load.start()

    def view(i, h):
        return g_l.at[2 * i + net.k, rows_of(0, rows, h), :]

    passed = [net.send(g, view(net.x, None), net.partner())]

    def arrived(i, h):
        passed.append(net.send(view(i, h), view(i, h), net.partner()))

    gather = ring(net, net.x, NX, net.at_x(1), net.at_x(-1), lambda h: g.at[rows_of(0, rows, h), :], view, arrived)
    next(gather)
    load.wait()
    store = pltpu.make_async_copy(buf, view(net.x, None), sem)
    store.start()
    yield from gather
    yield
    store.wait()
    for copy in passed:
        copy.wait_recv()


def layer_x(net, xf, x_l, buf, tmp, sem):
    rows, cols = buf.shape
    base = pl.multiple_of(net.k * rows, rows)

    def piece(i, h):
        return xf.at[rows_of(base, rows, h), pl.ds(pl.multiple_of(i * cols, cols), cols)]

    def slot(j, side, h):
        return x_l.at[2 * j + net.k, rows_of(0, rows, h), :]

    load = pltpu.make_async_copy(piece(net.x, None), buf, sem)
    load.start()
    own = slot(net.x, 0, None)
    passed = [net.send(piece(net.x, None), own, net.partner())]

    def arrived(j):
        passed.append(net.send(slot(j, 0, None), slot(j, 0, None), net.partner()))

    moves = exchange(net, net.x, NX, net.at_x(1), net.at_x(-1), piece, slot, tmp, arrived)
    next(moves)
    load.wait()
    store = pltpu.make_async_copy(buf, own, sem)
    store.start()
    yield
    yield from moves
    yield
    store.wait()
    for copy in passed:
        copy.wait_recv()


def gather_dpre(net, d_pre, col, d_pre_l, buf, sem):
    rows, cols = buf.shape
    cs = pl.ds(col * cols, cols)
    load = pltpu.make_async_copy(d_pre.at[:, cs], buf, sem)
    load.start()
    size = rows // 4

    def view(i, q):
        return d_pre_l.at[i, pl.ds(q * size, size), :]

    gather = ring(
        net, net.x, NX, net.at_x(1), net.at_x(-1), lambda q: d_pre.at[pl.ds(q * size, size), cs], view, lambda i, q: None, 4)
    next(gather)
    next(gather)
    load.wait()
    store = pltpu.make_async_copy(buf, d_pre_l.at[net.x], sem)
    store.start()
    yield
    yield from gather
    store.wait()


def exchange_sums(net, part, dst, tmp):
    rows, cols = dst.shape[1:]

    def piece(i, h):
        return part.at[rows_of(0, rows, h), pl.ds(pl.multiple_of(i * cols, cols), cols)]

    yield from exchange(
        net, net.y, NY, net.at_y(1), net.at_y(-1), piece, lambda j, side, h: dst.at[side, rows_of(0, rows, h), :], tmp)


def run(flows):
    flows = list(flows)
    while flows:
        flows = [f for f in flows if next(f, flows) is not flows]


def first_gather(w1, w2, x, g, w1f, w2s, xf, gf, b1, mid, tx, ty, bx, bg, lsem, ssem, rsem):
    net = Net(ssem, rsem)
    one = gather_w1(net, w1, w1f, b1, lsem.at[0])
    next(one)
    two = move_w2(net, w2, w2s, mid, tx, ty, lsem.at[3])
    next(two)
    next(one)
    tokens = [gather_tokens(net, x, xf, bx, lsem.at[1]), gather_tokens(net, g, gf, bg, lsem.at[2])]
    for f in tokens:
        next(f)
    next(two)
    next(one)
    run([two] + tokens + [one])
    net.finish()


def second_gather(w2s, act, g, w2f, act_l, g_l, b2, mid, tx, ty, bg, lsem, ssem, rsem):
    net = Net(ssem, rsem)
    acts = move_act(net, act, act_l, mid, tx, ty, lsem.at[1])
    next(acts)
    two = gather_w2(net, w2s, w2f, b2, lsem.at[0])
    next(two)
    next(acts)
    next(acts)
    next(acts)
    next(two)
    next(acts)
    toks = layer_g(net, g, g_l, bg, lsem.at[2])
    run([two, acts, toks])
    net.finish()


def third_gather(d_pre, xf, ys, d_pre_l, x_l, yb, bd, bx, tx, ty, lsem, ssem, rsem):
    net = Net(ssem, rsem)
    sums = exchange_sums(net, ys, yb, ty)
    next(sums)
    dp = gather_dpre(net, d_pre, 0, d_pre_l, bd, lsem.at[0])
    next(dp)
    toks = layer_x(net, xf, x_l, bx, tx, lsem.at[1])
    next(toks)
    run([dp, toks, sums])
    net.finish()


def fourth_gather(d_pre, dxs, d_pre_l, dxb, bd, ty, lsem, ssem, rsem):
    net = Net(ssem, rsem)
    sums = exchange_sums(net, dxs, dxb, ty)
    next(sums)
    dp = gather_dpre(net, d_pre, 1, d_pre_l, bd, lsem.at[0])
    run([dp, sums])
    net.finish()


def comm(body, outs, bufs, n_local, n_remote, *args):
    hbm = pl.BlockSpec(memory_space=pltpu.HBM)
    return pl.pallas_call(
        body,
        out_shape=[jax.ShapeDtypeStruct(s, d) for s, d in outs],
        in_specs=[hbm] * len(args),
        out_specs=[hbm] * len(outs),
        scratch_shapes=[pltpu.VMEM(s, d) for s, d in bufs] + [
            pltpu.SemaphoreType.DMA((n_local,)), pltpu.SemaphoreType.DMA((n_remote,)), pltpu.SemaphoreType.DMA((n_remote,))],
        compiler_params=pltpu.CompilerParams(has_side_effects=True),
        cost_estimate=pl.CostEstimate(flops=80_000_000_000, bytes_accessed=64 << 20, transcendentals=0),
    )(*args)


def solution(mesh):
    act_spec = P(("dep", "row"), "col")
    wgt_spec = P("row", "col")
    grad_spec = P(("row", "dep"), "col")
    bf16, f32 = jnp.bfloat16, jnp.float32
    swap = [(r, r ^ 1) for r in range(2 * NX)]

    def dot(a, b, dims):
        return lax.dot_general(a, b, (dims, ((), ())), preferred_element_type=f32)

    def local_block(x_loc, w_up, w_down, g_loc):
        tb, hb = x_loc.shape
        hr, fb = w_up.shape
        fk = fb // 2
        hid = NY * hb
        tok = 2 * tb
        k = lax.rem(lax.axis_index("row"), 2)
        y = lax.axis_index("col")

        w1f, w2s, xf, gf = comm(
            first_gather,
            [((2 * NX * hr, fk), bf16), ((fk // 8, hid), bf16), ((tok, hid), bf16), ((tok, hid), bf16)],
            [((hr, fk), bf16), ((4, fk // 8, hb), bf16), ((2, fk // 16, hb), bf16), ((2, fk // 16, hb), bf16),
             ((tb, hb), bf16), ((tb, hb), bf16)], 4, 80,
            w_up, w_down, x_loc, g_loc)
        pre_act = dot(xf, w1f, ((1,), (0,)))
        act = gelu_fwd(pre_act).astype(bf16)
        w2f, act_l, g_l = comm(
            second_gather,
            [((fk, hid), bf16), ((NX, 4, tok // 4, fk), bf16), ((2 * NX, tb, hb), bf16)],
            [((fk // 8, hid), bf16), ((4, tok // 4, fk), bf16), ((2, tok // 8, fk), bf16), ((2, tok // 8, fk), bf16),
             ((tb, hb), bf16)], 3, 80,
            w2s, act, g_loc)
        d_act = dot(gf, w2f, ((1,), (1,)))
        d_pre = (d_act * gelu_slope(pre_act)).astype(bf16)
        dw_down_part = dot(act_l.reshape(NX * tok, fk), g_l.reshape(NX * tok, hb), ((0,), (0,)))
        dw_down = lax.psum_scatter(dw_down_part, "dep", scatter_dimension=0, tiled=True)

        def core_sum(part):
            keep = lax.dynamic_slice_in_dim(part, k * tb, tb, 0)
            give = lax.dynamic_slice_in_dim(part, (1 - k) * tb, tb, 0)
            return keep + lax.ppermute(give, "row", swap)

        def col_sum(own, others):
            return (lax.dynamic_slice_in_dim(own, y * hb, hb, 1) + others[0] + others[1] + others[2]).astype(bf16)

        ys = core_sum(dot(act, w2f, ((1,), (0,))))
        d_pre, dw_down_part = lax.optimization_barrier((d_pre, dw_down_part))
        d_pre_l0, x_l, yb = comm(
            third_gather,
            [((NX, tok, fk // 2), bf16), ((2 * NX, tb, hb), bf16), ((3, tb, hb), f32)],
            [((tok, fk // 2), bf16), ((tb, hb), bf16), ((2, tb // 2, hb), bf16), ((2, tb // 2, hb), f32)], 2, 64,
            d_pre, xf, ys)
        x_l = x_l.reshape(NX * tok, 2, NZ, hr // NZ).transpose(0, 2, 1, 3).reshape(NX * tok, hb)

        def up_part(d_pre_l):
            return dot(x_l, d_pre_l.reshape(NX * tok, fk // 2), ((0,), (0,)))

        part0 = up_part(d_pre_l0)
        dxs = core_sum(dot(d_pre, w1f, ((1,), (1,))))
        d_pre, part0 = lax.optimization_barrier((d_pre, part0))
        d_pre_l1, dxb = comm(
            fourth_gather,
            [((NX, tok, fk // 2), bf16), ((3, tb, hb), f32)],
            [((tok, fk // 2), bf16), ((2, tb // 2, hb), f32)], 1, 40,
            d_pre, dxs)
        part0, dw_down = lax.optimization_barrier((part0, dw_down))
        outs = []
        for part in (part0, up_part(d_pre_l1)):
            total = lax.psum_scatter(part, "dep", scatter_dimension=0, tiled=True).reshape(2, hr // NZ, fk // 2)
            keep = jnp.where(k == 0, total[0], total[1])
            take = lax.ppermute(jnp.where(k == 0, total[1], total[0]), "row", swap)
            outs.append((jnp.where(k == 0, keep, take), jnp.where(k == 0, take, keep)))
        dw_up = jnp.concatenate([outs[0][0], outs[1][0], outs[0][1], outs[1][1]], axis=1)
        return col_sum(ys, yb), col_sum(dxs, dxb), dw_up, dw_down

    return jax.shard_map(local_block, mesh=mesh, in_specs=(act_spec, wgt_spec, wgt_spec, act_spec), out_specs=(act_spec, act_spec, grad_spec, grad_spec), check_vma=False)
```

```python
import jax
import jax.numpy as jnp
from jax import lax
from jax.experimental import pallas as pl
from jax.experimental.pallas import tpu as pltpu
from jax.sharding import PartitionSpec as P

GELU_COEF = 0.7978845608028654
CUBIC_COEF = 0.044715
NX = 4
NY = 4
NZ = 4


def gelu_fwd(pre_act):
    inner = GELU_COEF * (pre_act + CUBIC_COEF * pre_act * pre_act * pre_act)
    return 0.5 * pre_act * (1.0 + jnp.tanh(inner))


def gelu_slope(pre_act):
    inner = GELU_COEF * (pre_act + CUBIC_COEF * pre_act * pre_act * pre_act)
    tanh_val = jnp.tanh(inner)
    return 0.5 * (1.0 + tanh_val) + 0.5 * pre_act * (1.0 - tanh_val * tanh_val) * GELU_COEF * (1.0 + 3.0 * CUBIC_COEF * pre_act * pre_act)


def rot(v, d, n):
    return lax.rem(v + (d % n), n)


class Net:
    def __init__(self, send_sem, recv_sem):
        self.send_sem, self.recv_sem = send_sem, recv_sem
        self.used = 0
        self.sent = []
        self.z = lax.axis_index("dep")
        self.y = lax.axis_index("col")
        row = lax.axis_index("row")
        self.row = row
        self.x = lax.div(row, 2)
        self.k = lax.rem(row, 2)

    def slots(self, n):
        base = self.used
        self.used += n
        return base

    def make(self, src, dst, where, send_slot, recv_slot):
        return pltpu.make_async_remote_copy(
            src_ref=src, dst_ref=dst, send_sem=self.send_sem.at[send_slot], recv_sem=self.recv_sem.at[recv_slot],
            device_id=where, device_id_type=pl.DeviceIdType.MESH)

    def send(self, src, dst, where):
        slot = self.slots(1)
        copy = self.make(src, dst, where, slot, slot)
        copy.start()
        self.sent.append(copy)
        return copy

    def finish(self):
        for copy in self.sent:
            copy.wait_send()

    def at_x(self, d):
        return {"row": 2 * rot(self.x, d, NX) + self.k}

    def at_y(self, d):
        return {"col": rot(self.y, d, NY)}

    def at_z(self, d):
        return {"dep": rot(self.z, d, NZ)}

    def partner(self):
        return {"row": 2 * self.x + 1 - self.k}


def ring(net, place, n, up, down, own, view, arrived, pieces=2):
    west, east, far = rot(place, -1, n), rot(place, 1, n), rot(place, 2, n)
    ups, downs, relays = [], [], []
    for q in range(pieces):
        if q == pieces // 2:
            yield
        r = pieces - 1 - q
        ups.append(net.send(own(q), view(place, q), up))
        downs.append(net.send(own(r), view(place, r), down))
    for q in range(pieces):
        yield
        r = pieces - 1 - q
        ups[q].wait_recv()
        if q < pieces // 2:
            relays.append((q, net.send(view(west, q), view(west, q), up)))
        arrived(west, q)
        downs[q].wait_recv()
        if q < pieces // 2:
            relays.append((r, net.send(view(east, r), view(east, r), down)))
        arrived(east, r)
    for q, copy in relays:
        yield
        copy.wait_recv()
        arrived(far, q)


def exchange(net, place, n, up, down, piece, slot, tmp, arrived=lambda j: None):
    west, east, far = rot(place, -1, n), rot(place, 1, n), rot(place, 2, n)
    lo = net.send(piece(far, 0), tmp.at[0], up)
    hi = net.send(piece(far, 1), tmp.at[1], down)
    e = net.send(piece(east, None), slot(place, 0, None), up)
    w = net.send(piece(west, None), slot(place, 1, None), down)
    yield
    lo.wait_recv()
    lo = net.send(tmp.at[0], slot(west, 2, 0), up)
    hi.wait_recv()
    hi = net.send(tmp.at[1], slot(east, 2, 1), down)
    yield
    e.wait_recv()
    arrived(west)
    w.wait_recv()
    arrived(east)
    yield
    lo.wait_recv()
    hi.wait_recv()
    arrived(far)


def rows_of(base, size, h):
    return pl.ds(base, size) if h is None else pl.ds(base + h * (size // 2), size // 2)


def to_z(net, view, got, pieces):
    def arrived(i, q):
        got.append(net.send(view(i, q), view(i, q), net.at_z(1 if q < pieces // 2 else -1)))
    return arrived


def gather_w1(net, w1, w1f, buf, sem):
    rows, cols = w1.shape[0], w1f.shape[1]
    size = rows // 4
    parity = lax.rem(net.z, 2)
    mine = pl.ds(pl.multiple_of(net.k * cols, cols), cols)
    other = pl.ds(pl.multiple_of((1 - net.k) * cols, cols), cols)

    def slot(i, q, k):
        return w1f.at[pl.ds(pl.multiple_of(i * 8 * size + q * 2 * size + k * size, size), size), :]

    load = pltpu.make_async_copy(w1.at[:, mine], buf, sem)
    load.start()
    swaps = [net.send(w1.at[pl.ds(q * size, size), other], slot(net.x, q, net.k), net.partner()) for q in range(4)]
    yield
    load.wait()
    stores = [pltpu.make_async_copy(buf.at[pl.ds(q * size, size), :], slot(net.x, q, net.k), sem) for q in range(4)]
    for copy in stores:
        copy.start()
    for copy in swaps:
        copy.wait_recv()
    for copy in stores:
        copy.wait()

    def view(i, q):
        return slot(i, q, parity)

    got = []
    yield from ring(net, net.x, NX, net.at_x(1), net.at_x(-1), lambda q: view(net.x, q), view, to_z(net, view, got, 4), 4)
    yield
    for copy in got:
        copy.wait_recv()


def gather_tokens(net, src, dst, buf, sem, order=None):
    rows, cols = src.shape
    base = pl.multiple_of(net.k * rows, rows)

    def view(j, h):
        return dst.at[rows_of(base, rows, h), pl.ds(pl.multiple_of(j * cols, cols), cols)]

    if order is None:
        loads = [pltpu.make_async_copy(src, buf, sem)]
    else:
        size = cols // len(order)
        loads = [
            pltpu.make_async_copy(src.at[:, pl.ds(b * size, size)], buf.at[:, pl.ds(n * size, size)], sem) for n, b in enumerate(order)]
    for copy in loads:
        copy.start()
    for copy in loads:
        copy.wait()
    src = buf
    passed = [net.send(src, view(net.y, None), net.partner())]

    def arrived(j, h):
        passed.append(net.send(view(j, h), view(j, h), net.partner()))

    gather = ring(net, net.y, NY, net.at_y(1), net.at_y(-1), lambda h: src.at[rows_of(0, rows, h), :], view, arrived)
    next(gather)
    store = pltpu.make_async_copy(buf, view(net.y, None), sem)
    store.start()
    yield from gather
    yield
    store.wait()
    for copy in passed:
        copy.wait_recv()


def move_w2(net, w2, w2s, mid, tx, ty, sem):
    rows, cols = w2.shape
    part = rows // 8
    base = pl.multiple_of(lax.rem(net.z, 2) * 4 * part, part)

    def piece(i, h):
        return w2.at[rows_of(pl.multiple_of(base + i * part, part), part, h), :]

    load = pltpu.make_async_copy(piece(net.x, None), mid.at[net.x], sem)
    load.start()
    yield from exchange(net, net.x, NX, net.at_x(1), net.at_x(-1), piece, lambda j, side, h: mid.at[j, rows_of(0, part, h), :], tx)
    load.wait()

    def slot(j, side, h):
        return w2s.at[rows_of(0, part, h), pl.ds(pl.multiple_of(j * cols, cols), cols)]

    store = pltpu.make_async_copy(mid.at[net.y], slot(net.y, 0, None), sem)
    store.start()
    yield from exchange(net, net.y, NY, net.at_y(1), net.at_y(-1), lambda i, h: mid.at[i, rows_of(0, part, h), :], slot, ty)
    store.wait()


def gather_w2(net, w2s, w2f, sem):
    rows = w2s.shape[0]
    size = rows // 4
    base = lax.rem(net.z, 2) * 4 * rows

    def view(i, q):
        return w2f.at[pl.ds(pl.multiple_of(base + i * rows + q * size, size), size), :]

    def own(q):
        return w2s.at[pl.ds(q * size, size), :]

    got = []
    gather = ring(net, net.x, NX, net.at_x(1), net.at_x(-1), own, view, to_z(net, view, got, 4), 4)
    next(gather)
    for q in (0, 3, 1, 2):
        got.append(net.send(own(q), view(net.x, q), net.at_z(1 if q < 2 else -1)))
    store = pltpu.make_async_copy(w2s, w2f.at[pl.ds(pl.multiple_of(base + net.x * rows, rows), rows), :], sem)
    store.start()
    yield
    yield from gather
    yield
    for copy in got:
        copy.wait_recv()
    store.wait()


def move_act(net, act, act_l, cs, mid, tx, ty, sem):
    part = act_l.shape[2]

    def piece(i, h):
        return act.at[rows_of(pl.multiple_of(i * part, part), part, h), cs]

    load = pltpu.make_async_copy(piece(net.y, None), mid.at[net.y], sem)
    load.start()
    yield from exchange(net, net.y, NY, net.at_y(1), net.at_y(-1), piece, lambda j, side, h: mid.at[j, rows_of(0, part, h), :], ty)
    load.wait()
    store = pltpu.make_async_copy(mid.at[net.x], act_l.at[net.x, net.y, :, cs], sem)
    store.start()
    yield from exchange(
        net, net.x, NX, net.at_x(1), net.at_x(-1), lambda i, h: mid.at[i, rows_of(0, part, h), :],
        lambda j, side, h: act_l.at[j, net.y, rows_of(0, part, h), cs], tx)
    store.wait()

    def view(j, h):
        return act_l.at[pl.ds(2 * h, 2), j, :, cs]

    yield from ring(net, net.y, NY, net.at_y(1), net.at_y(-1), lambda h: view(net.y, h), view, lambda i, h: None)


def layer_g(net, g, g_l, buf, sem):
    rows = g.shape[0]
    load = pltpu.make_async_copy(g, buf, sem)
    load.start()

    def view(i, h):
        return g_l.at[2 * i + net.k, rows_of(0, rows, h), :]

    passed = [net.send(g, view(net.x, None), net.partner())]

    def arrived(i, h):
        passed.append(net.send(view(i, h), view(i, h), net.partner()))

    gather = ring(net, net.x, NX, net.at_x(1), net.at_x(-1), lambda h: g.at[rows_of(0, rows, h), :], view, arrived)
    next(gather)
    load.wait()
    store = pltpu.make_async_copy(buf, view(net.x, None), sem)
    store.start()
    yield from gather
    yield
    store.wait()
    for copy in passed:
        copy.wait_recv()


def layer_x(net, xf, x_l, buf, tmp, sem):
    rows, cols = buf.shape
    base = pl.multiple_of(net.k * rows, rows)

    def piece(i, h):
        return xf.at[rows_of(base, rows, h), pl.ds(pl.multiple_of(i * cols, cols), cols)]

    def slot(j, side, h):
        return x_l.at[2 * j + net.k, rows_of(0, rows, h), :]

    load = pltpu.make_async_copy(piece(net.x, None), buf, sem)
    load.start()
    own = slot(net.x, 0, None)
    passed = [net.send(piece(net.x, None), own, net.partner())]

    def arrived(j):
        passed.append(net.send(slot(j, 0, None), slot(j, 0, None), net.partner()))

    moves = exchange(net, net.x, NX, net.at_x(1), net.at_x(-1), piece, slot, tmp, arrived)
    next(moves)
    load.wait()
    store = pltpu.make_async_copy(buf, own, sem)
    store.start()
    yield
    yield from moves
    yield
    store.wait()
    for copy in passed:
        copy.wait_recv()


def gather_dpre(net, d_pre, col, d_pre_l, buf, sem):
    rows, cols = buf.shape
    cs = pl.ds(col * cols, cols)
    load = pltpu.make_async_copy(d_pre.at[:, cs], buf, sem)
    load.start()
    size = rows // 4

    def view(i, q):
        return d_pre_l.at[i, pl.ds(q * size, size), :]

    gather = ring(
        net, net.x, NX, net.at_x(1), net.at_x(-1), lambda q: d_pre.at[pl.ds(q * size, size), cs], view, lambda i, q: None, 4)
    next(gather)
    next(gather)
    load.wait()
    store = pltpu.make_async_copy(buf, d_pre_l.at[net.x], sem)
    store.start()
    yield
    yield from gather
    store.wait()


def exchange_sums(net, part, dst, tmp):
    rows, cols = dst.shape[1:]

    def piece(i, h):
        return part.at[rows_of(0, rows, h), pl.ds(pl.multiple_of(i * cols, cols), cols)]

    yield from exchange(
        net, net.y, NY, net.at_y(1), net.at_y(-1), piece, lambda j, side, h: dst.at[side, rows_of(0, rows, h), :], tmp)


def exchange_layers(net, part, dst, tmp):
    rows = dst.shape[1]

    def piece(i, h):
        return part.at[rows_of(pl.multiple_of(i * rows, rows), rows, h), :]

    yield from exchange(
        net, net.z, NZ, net.at_z(1), net.at_z(-1), piece, lambda j, side, h: dst.at[side, rows_of(0, rows, h), :], tmp)


def run(flows):
    flows = list(flows)
    while flows:
        flows = [f for f in flows if next(f, flows) is not flows]


def up_tiles(first, w1f, xv, wbuf, uv, av, wsem):
    cols = wbuf.shape[2]

    def fetch(i, slot):
        t = pl.ds(pl.multiple_of((first + i) * cols, cols), cols)
        return pltpu.make_async_copy(w1f.at[:, t], wbuf.at[slot], wsem.at[slot])

    fetch(0, 0).start()

    @pl.loop(0, 4)
    def _(i):
        slot = lax.rem(i, 2)

        @pl.when(i < 3)
        def _():
            fetch(i + 1, 1 - slot).start()

        fetch(i, slot).wait()
        t = pl.ds(pl.multiple_of((first + i) * cols, cols), cols)
        u = jnp.dot(xv[...], wbuf[slot], preferred_element_type=jnp.float32)
        uv[:, t] = u
        av[:, t] = gelu_fwd(u).astype(av.dtype)


def steps(flow, n):
    for _ in range(n):
        next(flow, None)


def first_kernel(
        w1, w2, x, g, w1f, w2f, xf, gf, pre, act, act_l, g_l, b1, mid, tx, ty, bx, bg, bl, w2s, xv, wbuf, uv, av, mids, txa, tya,
        lsem, wsem, ssem, rsem):
    net = Net(ssem, rsem)
    cols = act.shape[1] // 2
    chunks = [pl.ds(c * cols, cols) for c in range(2)]
    one = gather_w1(net, w1, w1f, b1, lsem.at[0])
    steps(one, 1)
    tokens = [gather_tokens(net, x, xf, bx, lsem.at[1], [c * NZ + q for q in range(NZ) for c in range(2)]), gather_tokens(net, g, gf, bg, lsem.at[2])]
    for f in tokens:
        steps(f, 1)
    steps(one, 2)
    two = move_w2(net, w2, w2s, mid, tx, ty, lsem.at[3])
    steps(two, 1)
    for f in tokens:
        steps(f, 2)
    steps(one, 1)
    for f in tokens:
        steps(f, 2)
    steps(one, 1)
    run(tokens)
    fetch = pltpu.make_async_copy(xf, xv, lsem.at[1])
    fetch.start()
    steps(two, 1)
    steps(one, 2)
    steps(two, 2)
    toks = layer_g(net, g, g_l, bl, lsem.at[2])
    steps(toks, 1)
    steps(one, 2)
    steps(two, 1)
    steps(one, 2)
    steps(two, 1)
    steps(toks, 1)
    steps(one, 2)
    run([two])
    three = gather_w2(net, w2s, w2f, lsem.at[3])
    steps(three, 1)
    run([one])
    fetch.wait()
    acts = []
    for c in range(2):
        up_tiles(4 * c, w1f, xv, wbuf, uv, av, wsem)
        keep_a = pltpu.make_async_copy(av.at[:, chunks[c]], act.at[:, chunks[c]], lsem.at[0])
        keep_u = pltpu.make_async_copy(uv.at[:, chunks[c]], pre.at[:, chunks[c]], lsem.at[1])
        keep_a.start()
        keep_u.start()
        keep_a.wait()
        acts.append(move_act(net, act, act_l, chunks[c], mids.at[c], txa.at[c], tya.at[c], lsem.at[4 + c]))
        steps(acts[c], 1)
        keep_u.wait()
    for n in (1, 2):
        steps(acts[0], n)
        steps(acts[1], n)
    steps(three, 1)
    for f in acts:
        steps(f, 1)
    steps(three, 1)
    for f in acts:
        steps(f, 2)
    run([three] + acts + [toks])
    net.finish()


def third_gather(d_pre, xf, ys, d_pre_l, x_l, yb, bd, bx, tx, ty, lsem, ssem, rsem):
    net = Net(ssem, rsem)
    sums = exchange_sums(net, ys, yb, ty)
    next(sums)
    dp = gather_dpre(net, d_pre, 0, d_pre_l, bd, lsem.at[0])
    next(dp)
    toks = layer_x(net, xf, x_l, bx, tx, lsem.at[1])
    next(toks)
    run([dp, toks, sums])
    net.finish()


def fourth_gather(d_pre, dxs, part, d_pre_l, dxb, part_b, bd, ty, tz, lsem, ssem, rsem):
    net = Net(ssem, rsem)
    ups = exchange_layers(net, part, part_b, tz)
    steps(ups, 1)
    sums = exchange_sums(net, dxs, dxb, ty)
    steps(sums, 1)
    dp = gather_dpre(net, d_pre, 1, d_pre_l, bd, lsem.at[0])
    run([dp, ups, sums])
    net.finish()


def blocks(a, order):
    size = a.shape[1] // len(order)
    return jnp.concatenate([a[:, b * size:(b + 1) * size] for b in order], axis=1)


def comm(body, outs, bufs, n_local, n_remote, *args):
    hbm = pl.BlockSpec(memory_space=pltpu.HBM)
    return pl.pallas_call(
        body,
        out_shape=[jax.ShapeDtypeStruct(s, d) for s, d in outs],
        in_specs=[hbm] * len(args),
        out_specs=[hbm] * len(outs),
        scratch_shapes=[pltpu.VMEM(s, d) for s, d in bufs] + [
            pltpu.SemaphoreType.DMA((n,)) for n in (*n_local, n_remote, n_remote)],
        compiler_params=pltpu.CompilerParams(has_side_effects=True),
        cost_estimate=pl.CostEstimate(flops=80_000_000_000, bytes_accessed=64 << 20, transcendentals=0),
    )(*args)


def solution(mesh):
    act_spec = P(("dep", "row"), "col")
    wgt_spec = P("row", "col")
    grad_spec = P(("row", "dep"), "col")
    bf16, f32 = jnp.bfloat16, jnp.float32
    swap = [(r, r ^ 1) for r in range(2 * NX)]

    def dot(a, b, dims):
        return lax.dot_general(a, b, (dims, ((), ())), preferred_element_type=f32)

    def local_block(x_loc, w_up, w_down, g_loc):
        tb, hb = x_loc.shape
        hr, fb = w_up.shape
        fk = fb // 2
        hid = NY * hb
        tok = 2 * tb
        k = lax.rem(lax.axis_index("row"), 2)
        y = lax.axis_index("col")

        w1f, w2f, xf, gf, pre_act, act, act_l, g_l = comm(
            first_kernel,
            [((2 * NX * hr, fk), bf16), ((fk, hid), bf16), ((tok, hid), bf16), ((tok, hid), bf16), ((tok, fk), f32), ((tok, fk), bf16),
             ((NX, 4, tok // 4, fk), bf16), ((2 * NX, tb, hb), bf16)],
            [((hr, fk), bf16), ((4, fk // 8, hb), bf16), ((2, fk // 16, hb), bf16), ((2, fk // 16, hb), bf16),
             ((tb, hb), bf16), ((tb, hb), bf16), ((tb, hb), bf16), ((fk // 8, hid), bf16), ((tok, hid), bf16), ((2, hid, fk // 8), bf16),
             ((tok, fk), f32), ((tok, fk), bf16), ((2, 4, tok // 4, fk // 2), bf16), ((2, 2, tok // 8, fk // 2), bf16),
             ((2, 2, tok // 8, fk // 2), bf16)], (6, 2), 160,
            w_up, w_down, x_loc, g_loc)
        d_act = dot(gf, w2f, ((1,), (1,)))
        d_pre = (d_act * gelu_slope(pre_act)).astype(bf16)
        dw_down_part = dot(act_l.reshape(NX * tok, fk), g_l.reshape(NX * tok, hb), ((0,), (0,)))
        dw_down = lax.psum_scatter(dw_down_part, "dep", scatter_dimension=0, tiled=True)

        def core_sum(part):
            keep = lax.dynamic_slice_in_dim(part, k * tb, tb, 0)
            give = lax.dynamic_slice_in_dim(part, (1 - k) * tb, tb, 0)
            return keep + lax.ppermute(give, "row", swap)

        def col_sum(own, others):
            return (lax.dynamic_slice_in_dim(own, y * hb, hb, 1) + others[0] + others[1] + others[2]).astype(bf16)

        ys = core_sum(dot(act, w2f, ((1,), (0,))))
        d_pre, dw_down_part = lax.optimization_barrier((d_pre, dw_down_part))
        d_pre_l0, x_l, yb = comm(
            third_gather,
            [((NX, tok, fk // 2), bf16), ((2 * NX, tb, hb), bf16), ((3, tb, hb), f32)],
            [((tok, fk // 2), bf16), ((tb, hb), bf16), ((2, tb // 2, hb), bf16), ((2, tb // 2, hb), f32)], (2,), 64,
            d_pre, xf, ys)
        x_l = x_l.reshape(NX * tok, hb)

        def up_part(d_pre_l):
            return dot(x_l, d_pre_l.reshape(NX * tok, fk // 2), ((0,), (0,)))

        part0 = up_part(d_pre_l0)
        dxs = core_sum(dot(d_pre, w1f, ((1,), (1,))))
        d_pre_l1, dxb, part_b = comm(
            fourth_gather,
            [((NX, tok, fk // 2), bf16), ((3, tb, hb), f32), ((3, 2 * hr // NZ, fk // 2), f32)],
            [((tok, fk // 2), bf16), ((2, tb // 2, hb), f32), ((2, hr // NZ, fk // 2), f32)], (1,), 40,
            d_pre, dxs, part0)
        own = lax.dynamic_slice_in_dim(part0, lax.axis_index("dep") * (2 * hr // NZ), 2 * hr // NZ, 0)
        totals = [own + part_b[0] + part_b[1] + part_b[2],
                  lax.psum_scatter(up_part(d_pre_l1), "dep", scatter_dimension=0, tiled=True)]
        outs = []
        for total in totals:
            total = total.reshape(2, hr // NZ, fk // 2)
            keep = jnp.where(k == 0, total[0], total[1])
            take = lax.ppermute(jnp.where(k == 0, total[1], total[0]), "row", swap)
            outs.append((jnp.where(k == 0, keep, take), jnp.where(k == 0, take, keep)))
        dw_up = jnp.concatenate([outs[0][0], outs[1][0], outs[0][1], outs[1][1]], axis=1)
        natural = [2 * q + c for c in range(2) for q in range(NZ)]
        return col_sum(ys, yb), blocks(col_sum(dxs, dxb), natural), dw_up, dw_down

    return jax.shard_map(local_block, mesh=mesh, in_specs=(act_spec, wgt_spec, wgt_spec, act_spec), out_specs=(act_spec, act_spec, grad_spec, grad_spec), check_vma=False)
```

```python
import jax
import jax.numpy as jnp
from jax import lax
from jax.experimental import pallas as pl
from jax.experimental.pallas import tpu as pltpu
from jax.sharding import PartitionSpec as P

GELU_COEF = 0.7978845608028654
CUBIC_COEF = 0.044715
NX = 4
NY = 4
NZ = 4
FIRST_ORDER = (0, 2, 3, 1, 6, 8, 4, 2, 3, 3, 2, 2, 3, 3, 3, 2, 6, 2, 2, 2, 6, 5, 5, 3, 8, 5, 5, 5, 5, 3, 2, 4, 0, 4, 0, 1, 8, 4, 0, 0, 1, 0, 1, 0, 8, 1, 0, 1, 6, 3, 3, 7, 1, 6, 1, 0, 0, 3, 3, 3, 1, 7, 7, 1, 7, 7, 0, 3, 1)
THIRD_ORDER = (1, 2, 0, 1, 0, 1, 2, 1, 2, 0, 0, 0, 2, 1, 1, 1)
FOURTH_ORDER = (0, 1, 2, 0, 1, 2, 2, 1, 2, 0, 2, 2, 2, 0, 1)


def gelu_fwd(pre_act):
    inner = GELU_COEF * (pre_act + CUBIC_COEF * pre_act * pre_act * pre_act)
    return 0.5 * pre_act * (1.0 + jnp.tanh(inner))


def gelu_slope(pre_act):
    inner = GELU_COEF * (pre_act + CUBIC_COEF * pre_act * pre_act * pre_act)
    tanh_val = jnp.tanh(inner)
    return 0.5 * (1.0 + tanh_val) + 0.5 * pre_act * (1.0 - tanh_val * tanh_val) * GELU_COEF * (1.0 + 3.0 * CUBIC_COEF * pre_act * pre_act)


def rot(v, d, n):
    return lax.rem(v + (d % n), n)


class Net:
    def __init__(self, send_sem, recv_sem):
        self.send_sem, self.recv_sem = send_sem, recv_sem
        self.used = 0
        self.sent = []
        self.z = lax.axis_index("dep")
        self.y = lax.axis_index("col")
        row = lax.axis_index("row")
        self.row = row
        self.x = lax.div(row, 2)
        self.k = lax.rem(row, 2)

    def slots(self, n):
        base = self.used
        self.used += n
        return base

    def make(self, src, dst, where, send_slot, recv_slot):
        return pltpu.make_async_remote_copy(
            src_ref=src, dst_ref=dst, send_sem=self.send_sem.at[send_slot], recv_sem=self.recv_sem.at[recv_slot],
            device_id=where, device_id_type=pl.DeviceIdType.MESH)

    def send(self, src, dst, where):
        slot = self.slots(1)
        copy = self.make(src, dst, where, slot, slot)
        copy.start()
        self.sent.append(copy)
        return copy

    def finish(self):
        for copy in self.sent:
            copy.wait_send()

    def at_x(self, d):
        return {"row": 2 * rot(self.x, d, NX) + self.k}

    def at_y(self, d):
        return {"col": rot(self.y, d, NY)}

    def at_z(self, d):
        return {"dep": rot(self.z, d, NZ)}

    def partner(self):
        return {"row": 2 * self.x + 1 - self.k}


class Gate:
    opened = False


def need(*gates):
    assert all(gate.opened for gate in gates)


def ring(net, place, n, up, down, own, view, arrived, pieces=2):
    west, east, far = rot(place, -1, n), rot(place, 1, n), rot(place, 2, n)
    ups, downs, relays = [], [], []

    def give(q):
        r = pieces - 1 - q
        ups.append(net.send(own(q), view(place, q), up))
        downs.append(net.send(own(r), view(place, r), down))

    give(0)
    give(1)
    for q in range(pieces):
        yield [ups[q], downs[q]]
        r = pieces - 1 - q
        ups[q].wait_recv()
        downs[q].wait_recv()
        if q < pieces // 2:
            relays.append((q, net.send(view(west, q), view(west, q), up)))
            relays.append((r, net.send(view(east, r), view(east, r), down)))
        if q + 2 < pieces:
            give(q + 2)
        arrived(west, q)
        arrived(east, r)
    for n in range(0, len(relays), 2):
        yield [copy for _, copy in relays[n:n + 2]]
        for q, copy in relays[n:n + 2]:
            copy.wait_recv()
            arrived(far, q)


def exchange(net, place, n, up, down, piece, slot, tmp, arrived=lambda j: None):
    west, east, far = rot(place, -1, n), rot(place, 1, n), rot(place, 2, n)
    lo = net.send(piece(far, 0), tmp.at[0], up)
    hi = net.send(piece(far, 1), tmp.at[1], down)
    e = net.send(piece(east, None), slot(place, 0, None), up)
    w = net.send(piece(west, None), slot(place, 1, None), down)
    yield [lo, hi]
    lo.wait_recv()
    lo = net.send(tmp.at[0], slot(west, 2, 0), up)
    hi.wait_recv()
    hi = net.send(tmp.at[1], slot(east, 2, 1), down)
    yield [e, w]
    e.wait_recv()
    arrived(west)
    w.wait_recv()
    arrived(east)
    yield [lo, hi]
    lo.wait_recv()
    hi.wait_recv()
    arrived(far)


def rows_of(base, size, h):
    return pl.ds(base, size) if h is None else pl.ds(base + h * (size // 2), size // 2)


def to_z(net, view, got, pieces):
    def arrived(i, q):
        got.append(net.send(view(i, q), view(i, q), net.at_z(1 if q < pieces // 2 else -1)))
    return arrived


def gather_w1(net, w1, w1f, buf, sem):
    rows, cols = w1.shape[0], w1f.shape[1]
    size = rows // 4
    parity = lax.rem(net.z, 2)
    mine = pl.ds(pl.multiple_of(net.k * cols, cols), cols)
    other = pl.ds(pl.multiple_of((1 - net.k) * cols, cols), cols)

    def slot(i, q, k):
        return w1f.at[pl.ds(pl.multiple_of(i * 8 * size + q * 2 * size + k * size, size), size), :]

    load = pltpu.make_async_copy(w1.at[:, mine], buf, sem)
    load.start()
    swaps = [net.send(w1.at[pl.ds(q * size, size), other], slot(net.x, q, net.k), net.partner()) for q in range(4)]
    yield swaps
    load.wait()
    stores = [pltpu.make_async_copy(buf.at[pl.ds(q * size, size), :], slot(net.x, q, net.k), sem) for q in range(4)]
    for copy in stores:
        copy.start()
    for copy in swaps:
        copy.wait_recv()
    for copy in stores:
        copy.wait()

    def view(i, q):
        return slot(i, q, parity)

    got = []
    yield from ring(net, net.x, NX, net.at_x(1), net.at_x(-1), lambda q: view(net.x, q), view, to_z(net, view, got, 4), 4)
    yield got
    for copy in got:
        copy.wait_recv()


def gather_tokens(net, src, dst, buf, sem, order=None):
    rows, cols = src.shape
    base = pl.multiple_of(net.k * rows, rows)

    def view(j, h):
        return dst.at[rows_of(base, rows, h), pl.ds(pl.multiple_of(j * cols, cols), cols)]

    if order is None:
        loads = [pltpu.make_async_copy(src, buf, sem)]
    else:
        size = cols // len(order)
        loads = [
            pltpu.make_async_copy(src.at[:, pl.ds(b * size, size)], buf.at[:, pl.ds(n * size, size)], sem) for n, b in enumerate(order)]
    for copy in loads:
        copy.start()
    for copy in loads:
        copy.wait()
    src = buf
    passed = [net.send(src, view(net.y, None), net.partner())]

    def arrived(j, h):
        passed.append(net.send(view(j, h), view(j, h), net.partner()))

    gather = ring(net, net.y, NY, net.at_y(1), net.at_y(-1), lambda h: src.at[rows_of(0, rows, h), :], view, arrived)
    first = next(gather)
    store = pltpu.make_async_copy(buf, view(net.y, None), sem)
    store.start()
    yield first
    yield from gather
    yield passed
    store.wait()
    for copy in passed:
        copy.wait_recv()


def move_w2(net, w2, w2s, mid, tx, ty, sem):
    rows, cols = w2.shape
    part = rows // 8
    base = pl.multiple_of(lax.rem(net.z, 2) * 4 * part, part)

    def piece(i, h):
        return w2.at[rows_of(pl.multiple_of(base + i * part, part), part, h), :]

    load = pltpu.make_async_copy(piece(net.x, None), mid.at[net.x], sem)
    load.start()
    yield from exchange(net, net.x, NX, net.at_x(1), net.at_x(-1), piece, lambda j, side, h: mid.at[j, rows_of(0, part, h), :], tx)
    load.wait()

    def slot(j, side, h):
        return w2s.at[rows_of(0, part, h), pl.ds(pl.multiple_of(j * cols, cols), cols)]

    store = pltpu.make_async_copy(mid.at[net.y], slot(net.y, 0, None), sem)
    store.start()
    yield from exchange(net, net.y, NY, net.at_y(1), net.at_y(-1), lambda i, h: mid.at[i, rows_of(0, part, h), :], slot, ty)
    store.wait()


def gather_w2(net, w2s, w2f, sem):
    rows = w2s.shape[0]
    size = rows // 4
    base = lax.rem(net.z, 2) * 4 * rows

    def view(i, q):
        return w2f.at[pl.ds(pl.multiple_of(base + i * rows + q * size, size), size), :]

    def own(q):
        return w2s.at[pl.ds(q * size, size), :]

    got = []
    gather = ring(net, net.x, NX, net.at_x(1), net.at_x(-1), own, view, to_z(net, view, got, 4), 4)
    first = next(gather)
    store = pltpu.make_async_copy(w2s, w2f.at[pl.ds(pl.multiple_of(base + net.x * rows, rows), rows), :], sem)
    store.start()
    yield first
    yield from gather
    yield got
    for copy in got:
        copy.wait_recv()
    store.wait()


def layers_w2(net, w2s, w2f):
    rows = w2s.shape[0]
    size = rows // 4
    base = lax.rem(net.z, 2) * 4 * rows + net.x * rows
    for q in range(2):
        got = []
        for p, d in ((q, 1), (3 - q, -1)):
            got.append(net.send(w2s.at[pl.ds(p * size, size), :], w2f.at[pl.ds(pl.multiple_of(base + p * size, size), size), :], net.at_z(d)))
        yield got
        for copy in got:
            copy.wait_recv()


def move_act(net, act, act_l, cs, mid, tx, ty, sem):
    part = act_l.shape[2]

    def piece(i, h):
        return act.at[rows_of(pl.multiple_of(i * part, part), part, h), cs]

    load = pltpu.make_async_copy(piece(net.y, None), mid.at[net.y], sem)
    load.start()
    yield from exchange(net, net.y, NY, net.at_y(1), net.at_y(-1), piece, lambda j, side, h: mid.at[j, rows_of(0, part, h), :], ty)
    load.wait()
    store = pltpu.make_async_copy(mid.at[net.x], act_l.at[net.x, net.y, :, cs], sem)
    store.start()
    yield from exchange(
        net, net.x, NX, net.at_x(1), net.at_x(-1), lambda i, h: mid.at[i, rows_of(0, part, h), :],
        lambda j, side, h: act_l.at[j, net.y, rows_of(0, part, h), cs], tx)
    store.wait()

    def view(j, h):
        return act_l.at[pl.ds(2 * h, 2), j, :, cs]

    yield from ring(net, net.y, NY, net.at_y(1), net.at_y(-1), lambda h: view(net.y, h), view, lambda i, h: None)


def layer_g(net, g, g_l, buf, sem):
    rows = g.shape[0]
    load = pltpu.make_async_copy(g, buf, sem)
    load.start()

    def view(i, h):
        return g_l.at[2 * i + net.k, rows_of(0, rows, h), :]

    passed = [net.send(g, view(net.x, None), net.partner())]

    def arrived(i, h):
        passed.append(net.send(view(i, h), view(i, h), net.partner()))

    gather = ring(net, net.x, NX, net.at_x(1), net.at_x(-1), lambda h: g.at[rows_of(0, rows, h), :], view, arrived)
    first = next(gather)
    load.wait()
    store = pltpu.make_async_copy(buf, view(net.x, None), sem)
    store.start()
    yield first
    yield from gather
    yield passed
    store.wait()
    for copy in passed:
        copy.wait_recv()


def layer_x(net, xf, x_l, buf, tmp, sem):
    rows, cols = buf.shape
    base = pl.multiple_of(net.k * rows, rows)

    def piece(i, h):
        return xf.at[rows_of(base, rows, h), pl.ds(pl.multiple_of(i * cols, cols), cols)]

    def slot(j, side, h):
        return x_l.at[2 * j + net.k, rows_of(0, rows, h), :]

    load = pltpu.make_async_copy(piece(net.x, None), buf, sem)
    load.start()
    own = slot(net.x, 0, None)
    passed = [net.send(piece(net.x, None), own, net.partner())]

    def arrived(j):
        passed.append(net.send(slot(j, 0, None), slot(j, 0, None), net.partner()))

    moves = exchange(net, net.x, NX, net.at_x(1), net.at_x(-1), piece, slot, tmp, arrived)
    first = next(moves)
    load.wait()
    store = pltpu.make_async_copy(buf, own, sem)
    store.start()
    yield first
    yield from moves
    yield passed
    store.wait()
    for copy in passed:
        copy.wait_recv()


def gather_dpre(net, d_pre, col, d_pre_l, buf, sem):
    rows, cols = buf.shape
    cs = pl.ds(col * cols, cols)
    load = pltpu.make_async_copy(d_pre.at[:, cs], buf, sem)
    load.start()
    size = rows // 4

    def view(i, q):
        return d_pre_l.at[i, pl.ds(q * size, size), :]

    gather = ring(
        net, net.x, NX, net.at_x(1), net.at_x(-1), lambda q: d_pre.at[pl.ds(q * size, size), cs], view, lambda i, q: None, 4)
    first = next(gather)
    load.wait()
    store = pltpu.make_async_copy(buf, d_pre_l.at[net.x], sem)
    store.start()
    yield first
    yield from gather
    store.wait()


def exchange_sums(net, part, dst, tmp):
    rows, cols = dst.shape[1:]

    def piece(i, h):
        return part.at[rows_of(0, rows, h), pl.ds(pl.multiple_of(i * cols, cols), cols)]

    yield from exchange(
        net, net.y, NY, net.at_y(1), net.at_y(-1), piece, lambda j, side, h: dst.at[side, rows_of(0, rows, h), :], tmp)


def exchange_layers(net, part, dst, tmp):
    rows = dst.shape[1]

    def piece(i, h):
        return part.at[rows_of(pl.multiple_of(i * rows, rows), rows, h), :]

    yield from exchange(
        net, net.z, NZ, net.at_z(1), net.at_z(-1), piece, lambda j, side, h: dst.at[side, rows_of(0, rows, h), :], tmp)


def run(flows, order=()):
    for n in order:
        next(flows[n], None)
    flows = list(flows)
    while flows:
        flows = [f for f in flows if next(f, flows) is not flows]


def up_tiles(first, w1f, xv, wbuf, uv, av, wsem):
    cols = wbuf.shape[2]

    def fetch(i, slot):
        t = pl.ds(pl.multiple_of((first + i) * cols, cols), cols)
        return pltpu.make_async_copy(w1f.at[:, t], wbuf.at[slot], wsem.at[slot])

    fetch(0, 0).start()

    @pl.loop(0, 4)
    def _(i):
        slot = lax.rem(i, 2)

        @pl.when(i < 3)
        def _():
            fetch(i + 1, 1 - slot).start()

        fetch(i, slot).wait()
        t = pl.ds(pl.multiple_of((first + i) * cols, cols), cols)
        u = jnp.dot(xv[...], wbuf[slot], preferred_element_type=jnp.float32)
        uv[:, t] = u
        av[:, t] = gelu_fwd(u).astype(av.dtype)


def first_kernel(
        w1, w2, x, g, w1f, w2f, xf, gf, pre, act, act_l, g_l, b1, mid, tx, ty, bx, bg, bl, w2s, xv, wbuf, uv, av, mids, txa, tya,
        lsem, wsem, ssem, rsem):
    net = Net(ssem, rsem)
    cols = act.shape[1] // 2
    chunks = [pl.ds(c * cols, cols) for c in range(2)]
    w1_here, x_here, a_here, w2_moved = Gate(), Gate(), [Gate(), Gate()], Gate()

    def weights1():
        yield from gather_w1(net, w1, w1f, b1, lsem.at[0])
        w1_here.opened = True

    def tokens_x():
        yield from gather_tokens(net, x, xf, bx, lsem.at[1], [c * NZ + q for q in range(NZ) for c in range(2)])
        fetch = pltpu.make_async_copy(xf, xv, lsem.at[1])
        fetch.start()
        yield []
        fetch.wait()
        x_here.opened = True

    def weights2():
        yield from move_w2(net, w2, w2s, mid, tx, ty, lsem.at[3])
        w2_moved.opened = True
        yield from gather_w2(net, w2s, w2f, lsem.at[3])

    def up():
        yield [w1_here, x_here]
        need(w1_here, x_here)
        for c in range(2):
            up_tiles(4 * c, w1f, xv, wbuf, uv, av, wsem)
            keep_a = pltpu.make_async_copy(av.at[:, chunks[c]], act.at[:, chunks[c]], lsem.at[6])
            keep_u = pltpu.make_async_copy(uv.at[:, chunks[c]], pre.at[:, chunks[c]], lsem.at[7])
            keep_a.start()
            keep_u.start()
            keep_a.wait()
            keep_u.wait()
            a_here[c].opened = True
            yield []

    def acts(c):
        yield [a_here[c]]
        need(a_here[c])
        yield from move_act(net, act, act_l, chunks[c], mids.at[c], txa.at[c], tya.at[c], lsem.at[4 + c])

    def weights2_own():
        yield [w2_moved]
        need(w2_moved)
        yield from layers_w2(net, w2s, w2f)

    def layer():
        yield from layer_g(net, g, g_l, bl, lsem.at[8])

    flows = [acts(0), acts(1), weights1(), weights2(), up(), tokens_x(), gather_tokens(net, g, gf, bg, lsem.at[2]), layer(), weights2_own()]
    run(flows, FIRST_ORDER)
    net.finish()


def third_gather(d_pre, xf, ys, d_pre_l, x_l, yb, bd, bx, tx, ty, lsem, ssem, rsem):
    net = Net(ssem, rsem)
    run([layer_x(net, xf, x_l, bx, tx, lsem.at[1]), gather_dpre(net, d_pre, 0, d_pre_l, bd, lsem.at[0]), exchange_sums(net, ys, yb, ty)],
        THIRD_ORDER)
    net.finish()


def fourth_gather(d_pre, dxs, part, d_pre_l, dxb, part_b, bd, ty, tz, lsem, ssem, rsem):
    net = Net(ssem, rsem)
    run([exchange_layers(net, part, part_b, tz), exchange_sums(net, dxs, dxb, ty), gather_dpre(net, d_pre, 1, d_pre_l, bd, lsem.at[0])],
        FOURTH_ORDER)
    net.finish()


def blocks(a, order):
    size = a.shape[1] // len(order)
    return jnp.concatenate([a[:, b * size:(b + 1) * size] for b in order], axis=1)


def comm(body, outs, bufs, n_local, n_remote, *args):
    hbm = pl.BlockSpec(memory_space=pltpu.HBM)
    return pl.pallas_call(
        body,
        out_shape=[jax.ShapeDtypeStruct(s, d) for s, d in outs],
        in_specs=[hbm] * len(args),
        out_specs=[hbm] * len(outs),
        scratch_shapes=[pltpu.VMEM(s, d) for s, d in bufs] + [
            pltpu.SemaphoreType.DMA((n,)) for n in (*n_local, n_remote, n_remote)],
        compiler_params=pltpu.CompilerParams(has_side_effects=True),
        cost_estimate=pl.CostEstimate(flops=80_000_000_000, bytes_accessed=64 << 20, transcendentals=0),
    )(*args)


def solution(mesh):
    act_spec = P(("dep", "row"), "col")
    wgt_spec = P("row", "col")
    grad_spec = P(("row", "dep"), "col")
    bf16, f32 = jnp.bfloat16, jnp.float32
    swap = [(r, r ^ 1) for r in range(2 * NX)]

    def dot(a, b, dims):
        return lax.dot_general(a, b, (dims, ((), ())), preferred_element_type=f32)

    def local_block(x_loc, w_up, w_down, g_loc):
        tb, hb = x_loc.shape
        hr, fb = w_up.shape
        fk = fb // 2
        hid = NY * hb
        tok = 2 * tb
        k = lax.rem(lax.axis_index("row"), 2)
        y = lax.axis_index("col")

        w1f, w2f, xf, gf, pre_act, act, act_l, g_l = comm(
            first_kernel,
            [((2 * NX * hr, fk), bf16), ((fk, hid), bf16), ((tok, hid), bf16), ((tok, hid), bf16), ((tok, fk), f32), ((tok, fk), bf16),
             ((NX, 4, tok // 4, fk), bf16), ((2 * NX, tb, hb), bf16)],
            [((hr, fk), bf16), ((4, fk // 8, hb), bf16), ((2, fk // 16, hb), bf16), ((2, fk // 16, hb), bf16),
             ((tb, hb), bf16), ((tb, hb), bf16), ((tb, hb), bf16), ((fk // 8, hid), bf16), ((tok, hid), bf16), ((2, hid, fk // 8), bf16),
             ((tok, fk), f32), ((tok, fk), bf16), ((2, 4, tok // 4, fk // 2), bf16), ((2, 2, tok // 8, fk // 2), bf16),
             ((2, 2, tok // 8, fk // 2), bf16)], (9, 2), 160,
            w_up, w_down, x_loc, g_loc)
        d_act = dot(gf, w2f, ((1,), (1,)))
        d_pre = (d_act * gelu_slope(pre_act)).astype(bf16)
        dw_down_part = dot(act_l.reshape(NX * tok, fk), g_l.reshape(NX * tok, hb), ((0,), (0,)))
        dw_down = lax.psum_scatter(dw_down_part, "dep", scatter_dimension=0, tiled=True)

        def core_sum(part):
            keep = lax.dynamic_slice_in_dim(part, k * tb, tb, 0)
            give = lax.dynamic_slice_in_dim(part, (1 - k) * tb, tb, 0)
            return keep + lax.ppermute(give, "row", swap)

        def col_sum(own, others):
            return (lax.dynamic_slice_in_dim(own, y * hb, hb, 1) + others[0] + others[1] + others[2]).astype(bf16)

        ys = core_sum(dot(act, w2f, ((1,), (0,))))
        d_pre, dw_down_part = lax.optimization_barrier((d_pre, dw_down_part))
        d_pre_l0, x_l, yb = comm(
            third_gather,
            [((NX, tok, fk // 2), bf16), ((2 * NX, tb, hb), bf16), ((3, tb, hb), f32)],
            [((tok, fk // 2), bf16), ((tb, hb), bf16), ((2, tb // 2, hb), bf16), ((2, tb // 2, hb), f32)], (2,), 64,
            d_pre, xf, ys)
        x_l = x_l.reshape(NX * tok, hb)

        def up_part(d_pre_l):
            return dot(x_l, d_pre_l.reshape(NX * tok, fk // 2), ((0,), (0,)))

        part0 = up_part(d_pre_l0)
        dxs = core_sum(dot(d_pre, w1f, ((1,), (1,))))
        part0, dw_down = lax.optimization_barrier((part0, dw_down))
        d_pre_l1, dxb, part_b = comm(
            fourth_gather,
            [((NX, tok, fk // 2), bf16), ((3, tb, hb), f32), ((3, 2 * hr // NZ, fk // 2), f32)],
            [((tok, fk // 2), bf16), ((2, tb // 2, hb), f32), ((2, hr // NZ, fk // 2), f32)], (1,), 40,
            d_pre, dxs, part0)
        own = lax.dynamic_slice_in_dim(part0, lax.axis_index("dep") * (2 * hr // NZ), 2 * hr // NZ, 0)
        totals = [own + part_b[0] + part_b[1] + part_b[2],
                  lax.psum_scatter(up_part(d_pre_l1), "dep", scatter_dimension=0, tiled=True)]
        outs = []
        for total in totals:
            total = total.reshape(2, hr // NZ, fk // 2)
            keep = jnp.where(k == 0, total[0], total[1])
            take = lax.ppermute(jnp.where(k == 0, total[1], total[0]), "row", swap)
            outs.append((jnp.where(k == 0, keep, take), jnp.where(k == 0, take, keep)))
        dw_up = jnp.concatenate([outs[0][0], outs[1][0], outs[0][1], outs[1][1]], axis=1)
        natural = [2 * q + c for c in range(2) for q in range(NZ)]
        return col_sum(ys, yb), blocks(col_sum(dxs, dxb), natural), dw_up, dw_down

    return jax.shard_map(local_block, mesh=mesh, in_specs=(act_spec, wgt_spec, wgt_spec, act_spec), out_specs=(act_spec, act_spec, grad_spec, grad_spec), check_vma=False)
```

```python
import jax
import jax.numpy as jnp
from jax import lax
from jax.experimental import pallas as pl
from jax.experimental.pallas import tpu as pltpu
from jax.sharding import PartitionSpec as P

GELU_COEF = 0.7978845608028654
CUBIC_COEF = 0.044715
NX = 4
NY = 4
NZ = 4
FIRST_ORDER = (0, 2, 3, 1, 6, 8, 4, 2, 3, 3, 2, 2, 3, 3, 3, 2, 6, 2, 2, 2, 6, 5, 5, 3, 8, 5, 5, 5, 5, 3, 2, 4, 0, 4, 0, 1, 8, 4, 0, 0, 1, 0, 1, 0, 8, 1, 0, 1, 6, 3, 3, 7, 1, 6, 1, 0, 0, 3, 3, 3, 1, 7, 7, 1, 7, 7, 0, 3, 1)
THIRD_ORDER = (0, 2, 2, 0, 2, 1, 2, 2, 2, 2, 1, 1, 1, 0, 0, 2, 0, 1, 1, 1, 2, 2)
FOURTH_ORDER = (2, 2, 2, 0, 1, 2, 2, 1, 2, 0, 2, 1, 1, 2, 1, 1, 1, 0, 0, 2, 2)


def gelu_fwd(pre_act):
    inner = GELU_COEF * (pre_act + CUBIC_COEF * pre_act * pre_act * pre_act)
    return 0.5 * pre_act * (1.0 + jnp.tanh(inner))


def gelu_slope(pre_act):
    inner = GELU_COEF * (pre_act + CUBIC_COEF * pre_act * pre_act * pre_act)
    tanh_val = jnp.tanh(inner)
    return 0.5 * (1.0 + tanh_val) + 0.5 * pre_act * (1.0 - tanh_val * tanh_val) * GELU_COEF * (1.0 + 3.0 * CUBIC_COEF * pre_act * pre_act)


def rot(v, d, n):
    return lax.rem(v + (d % n), n)


class Net:
    def __init__(self, send_sem, recv_sem):
        self.send_sem, self.recv_sem = send_sem, recv_sem
        self.used = 0
        self.sent = []
        self.z = lax.axis_index("dep")
        self.y = lax.axis_index("col")
        row = lax.axis_index("row")
        self.row = row
        self.x = lax.div(row, 2)
        self.k = lax.rem(row, 2)

    def slots(self, n):
        base = self.used
        self.used += n
        return base

    def make(self, src, dst, where, send_slot, recv_slot):
        return pltpu.make_async_remote_copy(
            src_ref=src, dst_ref=dst, send_sem=self.send_sem.at[send_slot], recv_sem=self.recv_sem.at[recv_slot],
            device_id=where, device_id_type=pl.DeviceIdType.MESH)

    def send(self, src, dst, where):
        slot = self.slots(1)
        copy = self.make(src, dst, where, slot, slot)
        copy.start()
        self.sent.append(copy)
        return copy

    def finish(self):
        for copy in self.sent:
            copy.wait_send()

    def at_x(self, d):
        return {"row": 2 * rot(self.x, d, NX) + self.k}

    def at_y(self, d):
        return {"col": rot(self.y, d, NY)}

    def at_z(self, d):
        return {"dep": rot(self.z, d, NZ)}

    def partner(self):
        return {"row": 2 * self.x + 1 - self.k}


class Gate:
    opened = False


def need(*gates):
    assert all(gate.opened for gate in gates)


def ring(net, place, n, up, down, own, view, arrived, pieces=2):
    west, east, far = rot(place, -1, n), rot(place, 1, n), rot(place, 2, n)
    ups, downs, relays = [], [], []

    def give(q):
        r = pieces - 1 - q
        ups.append(net.send(own(q), view(place, q), up))
        downs.append(net.send(own(r), view(place, r), down))

    give(0)
    give(1)
    for q in range(pieces):
        yield [ups[q], downs[q]]
        r = pieces - 1 - q
        ups[q].wait_recv()
        downs[q].wait_recv()
        if q < pieces // 2:
            relays.append((q, net.send(view(west, q), view(west, q), up)))
            relays.append((r, net.send(view(east, r), view(east, r), down)))
        if q + 2 < pieces:
            give(q + 2)
        arrived(west, q)
        arrived(east, r)
    for n in range(0, len(relays), 2):
        yield [copy for _, copy in relays[n:n + 2]]
        for q, copy in relays[n:n + 2]:
            copy.wait_recv()
            arrived(far, q)


def exchange(net, place, n, up, down, piece, slot, tmp, arrived=lambda j: None):
    west, east, far = rot(place, -1, n), rot(place, 1, n), rot(place, 2, n)
    lo = net.send(piece(far, 0), tmp.at[0], up)
    hi = net.send(piece(far, 1), tmp.at[1], down)
    e = net.send(piece(east, None), slot(place, 0, None), up)
    w = net.send(piece(west, None), slot(place, 1, None), down)
    yield [lo, hi]
    lo.wait_recv()
    lo = net.send(tmp.at[0], slot(west, 2, 0), up)
    hi.wait_recv()
    hi = net.send(tmp.at[1], slot(east, 2, 1), down)
    yield [e, w]
    e.wait_recv()
    arrived(west)
    w.wait_recv()
    arrived(east)
    yield [lo, hi]
    lo.wait_recv()
    hi.wait_recv()
    arrived(far)


def rows_of(base, size, h):
    return pl.ds(base, size) if h is None else pl.ds(base + h * (size // 2), size // 2)


def to_z(net, view, got, pieces):
    def arrived(i, q):
        got.append(net.send(view(i, q), view(i, q), net.at_z(1 if q < pieces // 2 else -1)))
    return arrived


def gather_w1(net, w1, w1f, buf, sem):
    rows, cols = w1.shape[0], w1f.shape[1]
    size = rows // 4
    parity = lax.rem(net.z, 2)
    mine = pl.ds(pl.multiple_of(net.k * cols, cols), cols)
    other = pl.ds(pl.multiple_of((1 - net.k) * cols, cols), cols)

    def slot(i, q, k):
        return w1f.at[pl.ds(pl.multiple_of(i * 8 * size + q * 2 * size + k * size, size), size), :]

    load = pltpu.make_async_copy(w1.at[:, mine], buf, sem)
    load.start()
    swaps = [net.send(w1.at[pl.ds(q * size, size), other], slot(net.x, q, net.k), net.partner()) for q in range(4)]
    yield swaps
    load.wait()
    stores = [pltpu.make_async_copy(buf.at[pl.ds(q * size, size), :], slot(net.x, q, net.k), sem) for q in range(4)]
    for copy in stores:
        copy.start()
    for copy in swaps:
        copy.wait_recv()
    for copy in stores:
        copy.wait()

    def view(i, q):
        return slot(i, q, parity)

    got = []
    yield from ring(net, net.x, NX, net.at_x(1), net.at_x(-1), lambda q: view(net.x, q), view, to_z(net, view, got, 4), 4)
    yield got
    for copy in got:
        copy.wait_recv()


def gather_tokens(net, src, dst, buf, sem, order=None):
    rows, cols = src.shape
    base = pl.multiple_of(net.k * rows, rows)

    def view(j, h):
        return dst.at[rows_of(base, rows, h), pl.ds(pl.multiple_of(j * cols, cols), cols)]

    if order is None:
        loads = [pltpu.make_async_copy(src, buf, sem)]
    else:
        size = cols // len(order)
        loads = [
            pltpu.make_async_copy(src.at[:, pl.ds(b * size, size)], buf.at[:, pl.ds(n * size, size)], sem) for n, b in enumerate(order)]
    for copy in loads:
        copy.start()
    for copy in loads:
        copy.wait()
    src = buf
    passed = [net.send(src, view(net.y, None), net.partner())]

    def arrived(j, h):
        passed.append(net.send(view(j, h), view(j, h), net.partner()))

    gather = ring(net, net.y, NY, net.at_y(1), net.at_y(-1), lambda h: src.at[rows_of(0, rows, h), :], view, arrived)
    first = next(gather)
    store = pltpu.make_async_copy(buf, view(net.y, None), sem)
    store.start()
    yield first
    yield from gather
    yield passed
    store.wait()
    for copy in passed:
        copy.wait_recv()


def move_w2(net, w2, w2s, mid, tx, ty, sem):
    rows, cols = w2.shape
    part = rows // 8
    base = pl.multiple_of(lax.rem(net.z, 2) * 4 * part, part)

    def piece(i, h):
        return w2.at[rows_of(pl.multiple_of(base + i * part, part), part, h), :]

    load = pltpu.make_async_copy(piece(net.x, None), mid.at[net.x], sem)
    load.start()
    yield from exchange(net, net.x, NX, net.at_x(1), net.at_x(-1), piece, lambda j, side, h: mid.at[j, rows_of(0, part, h), :], tx)
    load.wait()

    def slot(j, side, h):
        return w2s.at[rows_of(0, part, h), pl.ds(pl.multiple_of(j * cols, cols), cols)]

    store = pltpu.make_async_copy(mid.at[net.y], slot(net.y, 0, None), sem)
    store.start()
    yield from exchange(net, net.y, NY, net.at_y(1), net.at_y(-1), lambda i, h: mid.at[i, rows_of(0, part, h), :], slot, ty)
    store.wait()


def gather_w2(net, w2s, w2f, sem):
    rows = w2s.shape[0]
    size = rows // 4
    base = lax.rem(net.z, 2) * 4 * rows

    def view(i, q):
        return w2f.at[pl.ds(pl.multiple_of(base + i * rows + q * size, size), size), :]

    def own(q):
        return w2s.at[pl.ds(q * size, size), :]

    got = []
    gather = ring(net, net.x, NX, net.at_x(1), net.at_x(-1), own, view, to_z(net, view, got, 4), 4)
    first = next(gather)
    store = pltpu.make_async_copy(w2s, w2f.at[pl.ds(pl.multiple_of(base + net.x * rows, rows), rows), :], sem)
    store.start()
    yield first
    yield from gather
    yield got
    for copy in got:
        copy.wait_recv()
    store.wait()


def layers_w2(net, w2s, w2f):
    rows = w2s.shape[0]
    size = rows // 4
    base = lax.rem(net.z, 2) * 4 * rows + net.x * rows
    for q in range(2):
        got = []
        for p, d in ((q, 1), (3 - q, -1)):
            got.append(net.send(w2s.at[pl.ds(p * size, size), :], w2f.at[pl.ds(pl.multiple_of(base + p * size, size), size), :], net.at_z(d)))
        yield got
        for copy in got:
            copy.wait_recv()


def move_act(net, act, act_l, cs, mid, tx, ty, sem):
    part = act_l.shape[2]

    def piece(i, h):
        return act.at[rows_of(pl.multiple_of(i * part, part), part, h), cs]

    load = pltpu.make_async_copy(piece(net.y, None), mid.at[net.y], sem)
    load.start()
    yield from exchange(net, net.y, NY, net.at_y(1), net.at_y(-1), piece, lambda j, side, h: mid.at[j, rows_of(0, part, h), :], ty)
    load.wait()
    store = pltpu.make_async_copy(mid.at[net.x], act_l.at[net.x, net.y, :, cs], sem)
    store.start()
    yield from exchange(
        net, net.x, NX, net.at_x(1), net.at_x(-1), lambda i, h: mid.at[i, rows_of(0, part, h), :],
        lambda j, side, h: act_l.at[j, net.y, rows_of(0, part, h), cs], tx)
    store.wait()

    def view(j, h):
        return act_l.at[pl.ds(2 * h, 2), j, :, cs]

    yield from ring(net, net.y, NY, net.at_y(1), net.at_y(-1), lambda h: view(net.y, h), view, lambda i, h: None)


def layer_g(net, g, g_l, buf, sem):
    rows = g.shape[0]
    load = pltpu.make_async_copy(g, buf, sem)
    load.start()

    def view(i, h):
        return g_l.at[2 * i + net.k, rows_of(0, rows, h), :]

    passed = [net.send(g, view(net.x, None), net.partner())]

    def arrived(i, h):
        passed.append(net.send(view(i, h), view(i, h), net.partner()))

    gather = ring(net, net.x, NX, net.at_x(1), net.at_x(-1), lambda h: g.at[rows_of(0, rows, h), :], view, arrived)
    first = next(gather)
    load.wait()
    store = pltpu.make_async_copy(buf, view(net.x, None), sem)
    store.start()
    yield first
    yield from gather
    yield passed
    store.wait()
    for copy in passed:
        copy.wait_recv()


def layer_x(net, xf, x_l, buf, tmp, sem):
    rows, cols = buf.shape
    base = pl.multiple_of(net.k * rows, rows)

    def piece(i, h):
        return xf.at[rows_of(base, rows, h), pl.ds(pl.multiple_of(i * cols, cols), cols)]

    def slot(j, side, h):
        return x_l.at[2 * j + net.k, rows_of(0, rows, h), :]

    load = pltpu.make_async_copy(piece(net.x, None), buf, sem)
    load.start()
    own = slot(net.x, 0, None)
    passed = [net.send(piece(net.x, None), own, net.partner())]

    def arrived(j):
        passed.append(net.send(slot(j, 0, None), slot(j, 0, None), net.partner()))

    moves = exchange(net, net.x, NX, net.at_x(1), net.at_x(-1), piece, slot, tmp, arrived)
    first = next(moves)
    load.wait()
    store = pltpu.make_async_copy(buf, own, sem)
    store.start()
    yield first
    yield from moves
    yield passed
    store.wait()
    for copy in passed:
        copy.wait_recv()


def gather_dpre(net, d_pre, col, d_pre_l, buf, sem):
    rows, cols = buf.shape
    cs = pl.ds(col * cols, cols)
    load = pltpu.make_async_copy(d_pre.at[:, cs], buf, sem)
    load.start()
    size = rows // 4

    def view(i, q):
        return d_pre_l.at[i, pl.ds(q * size, size), :]

    gather = ring(
        net, net.x, NX, net.at_x(1), net.at_x(-1), lambda q: d_pre.at[pl.ds(q * size, size), cs], view, lambda i, q: None, 4)
    first = next(gather)
    load.wait()
    store = pltpu.make_async_copy(buf, d_pre_l.at[net.x], sem)
    store.start()
    yield first
    yield from gather
    store.wait()


def block_tiles(out, lhs, w, base, by_rows, wbuf, wsem):
    size = out.shape[1] // 4

    def fetch(i, slot):
        t = pl.ds(pl.multiple_of(base + i * size, size), size)
        return pltpu.make_async_copy(w.at[t, :] if by_rows else w.at[:, t], wbuf.at[slot], wsem.at[slot])

    fetch(0, 0).start()

    @pl.loop(0, 4)
    def _(i):
        slot = lax.rem(i, 2)

        @pl.when(i < 3)
        def _():
            fetch(i + 1, 1 - slot).start()

        fetch(i, slot).wait()
        dims = (((1,), (1 if by_rows else 0,)), ((), ()))
        out[:, pl.ds(pl.multiple_of(i * size, size), size)] = lax.dot_general(
            lhs[...], wbuf[slot], dims, preferred_element_type=jnp.float32)


def add_own(got, own, k):
    rows = got.shape[0]

    @pl.loop(0, rows, step=16)
    def _(r):
        here = pl.ds(pl.multiple_of(r, 16), 16)
        got[here, :] += own[pl.ds(pl.multiple_of(k * rows + r, 16), 16), :]


def add_all(out, own, others, order):
    rows = out.shape[0]
    size = out.shape[1] // len(order)

    @pl.loop(0, rows, step=16)
    def _(r):
        here = pl.ds(pl.multiple_of(r, 16), 16)
        total = (own[here, :] + others[0, here, :] + others[1, here, :] + others[2, here, :]).astype(out.dtype)
        for n, b in enumerate(order):
            out[here, b * size:(b + 1) * size] = total[:, n * size:(n + 1) * size]


def summed(net, lhs, w, by_rows, dst, order, lv, wbuf, parts, got, others, tmp, out, sem, wsem):
    rows, cols = got.shape[1:]
    load = pltpu.make_async_copy(lhs, lv, sem)
    load.start()
    load.wait()
    other = pl.ds(pl.multiple_of((1 - net.k) * rows, rows), rows)
    up, down = net.at_y(1), net.at_y(-1)
    half = rows // 2
    lower, upper = pl.ds(0, half), pl.ds(half, half)
    swaps = []

    def part(n):
        base = rot(net.y, (2, 1, 3, 0)[n], NY) * cols
        block_tiles(parts.at[n], lv, w, base, by_rows, wbuf, wsem)
        swaps.append(net.send(parts.at[n, other], got.at[n], net.partner()))

    def add(n):
        swaps[n].wait_recv()
        add_own(got.at[n], parts.at[n], net.k)

    part(0)
    yield []
    part(1)
    yield [swaps[0]]
    add(0)
    part(2)
    lo = net.send(got.at[0, lower], tmp.at[0], up)
    hi = net.send(got.at[0, upper], tmp.at[1], down)
    yield [swaps[1]]
    add(1)
    part(3)
    e = net.send(got.at[1], others.at[0], up)
    yield [swaps[2]]
    add(2)
    yield [swaps[3]]
    add(3)
    w_ = net.send(got.at[2], others.at[1], down)
    yield [lo, hi]
    lo.wait_recv()
    lo = net.send(tmp.at[0], others.at[2, lower], up)
    hi.wait_recv()
    hi = net.send(tmp.at[1], others.at[2, upper], down)
    yield [e, w_]
    e.wait_recv()
    w_.wait_recv()
    yield [lo, hi]
    lo.wait_recv()
    hi.wait_recv()
    add_all(out, got.at[3], others, order)
    store = pltpu.make_async_copy(out, dst, sem)
    store.start()
    yield []
    store.wait()


def exchange_layers(net, part, dst, tmp):
    rows = dst.shape[1]

    def piece(i, h):
        return part.at[rows_of(pl.multiple_of(i * rows, rows), rows, h), :]

    yield from exchange(
        net, net.z, NZ, net.at_z(1), net.at_z(-1), piece, lambda j, side, h: dst.at[side, rows_of(0, rows, h), :], tmp)


def run(flows, order=()):
    for n in order:
        next(flows[n], None)
    flows = list(flows)
    while flows:
        flows = [f for f in flows if next(f, flows) is not flows]


def up_tiles(first, w1f, xv, wbuf, uv, av, wsem):
    cols = wbuf.shape[2]

    def fetch(i, slot):
        t = pl.ds(pl.multiple_of((first + i) * cols, cols), cols)
        return pltpu.make_async_copy(w1f.at[:, t], wbuf.at[slot], wsem.at[slot])

    fetch(0, 0).start()

    @pl.loop(0, 4)
    def _(i):
        slot = lax.rem(i, 2)

        @pl.when(i < 3)
        def _():
            fetch(i + 1, 1 - slot).start()

        fetch(i, slot).wait()
        t = pl.ds(pl.multiple_of((first + i) * cols, cols), cols)
        u = jnp.dot(xv[...], wbuf[slot], preferred_element_type=jnp.float32)
        uv[:, t] = u
        av[:, t] = gelu_fwd(u).astype(av.dtype)


def first_kernel(
        w1, w2, x, g, w1f, w2f, xf, gf, pre, act, act_l, g_l, b1, mid, tx, ty, bx, bg, bl, w2s, xv, wbuf, uv, av, mids, txa, tya,
        lsem, wsem, ssem, rsem):
    net = Net(ssem, rsem)
    cols = act.shape[1] // 2
    chunks = [pl.ds(c * cols, cols) for c in range(2)]
    w1_here, x_here, a_here, w2_moved = Gate(), Gate(), [Gate(), Gate()], Gate()

    def weights1():
        yield from gather_w1(net, w1, w1f, b1, lsem.at[0])
        w1_here.opened = True

    def tokens_x():
        yield from gather_tokens(net, x, xf, bx, lsem.at[1], [c * NZ + q for q in range(NZ) for c in range(2)])
        fetch = pltpu.make_async_copy(xf, xv, lsem.at[1])
        fetch.start()
        yield []
        fetch.wait()
        x_here.opened = True

    def weights2():
        yield from move_w2(net, w2, w2s, mid, tx, ty, lsem.at[3])
        w2_moved.opened = True
        yield from gather_w2(net, w2s, w2f, lsem.at[3])

    def up():
        yield [w1_here, x_here]
        need(w1_here, x_here)
        for c in range(2):
            up_tiles(4 * c, w1f, xv, wbuf, uv, av, wsem)
            keep_a = pltpu.make_async_copy(av.at[:, chunks[c]], act.at[:, chunks[c]], lsem.at[6])
            keep_u = pltpu.make_async_copy(uv.at[:, chunks[c]], pre.at[:, chunks[c]], lsem.at[7])
            keep_a.start()
            keep_u.start()
            keep_a.wait()
            keep_u.wait()
            a_here[c].opened = True
            yield []

    def acts(c):
        yield [a_here[c]]
        need(a_here[c])
        yield from move_act(net, act, act_l, chunks[c], mids.at[c], txa.at[c], tya.at[c], lsem.at[4 + c])

    def weights2_own():
        yield [w2_moved]
        need(w2_moved)
        yield from layers_w2(net, w2s, w2f)

    def layer():
        yield from layer_g(net, g, g_l, bl, lsem.at[8])

    flows = [acts(0), acts(1), weights1(), weights2(), up(), tokens_x(), gather_tokens(net, g, gf, bg, lsem.at[2]), layer(), weights2_own()]
    run(flows, FIRST_ORDER)
    net.finish()


def third_gather(
        d_pre, xf, act, w2f, d_pre_l, x_l, y_out, bd, bx, tx, lv, wbuf, parts, got, others, ty, out, lsem, wsem, ssem, rsem):
    net = Net(ssem, rsem)
    run([layer_x(net, xf, x_l, bx, tx, lsem.at[1]), gather_dpre(net, d_pre, 0, d_pre_l, bd, lsem.at[0]),
         summed(net, act, w2f, False, y_out, [0], lv, wbuf, parts, got, others, ty, out, lsem.at[2], wsem)], THIRD_ORDER)
    net.finish()


def fourth_gather(
        d_pre, w1f, part, d_pre_l, dx_out, part_b, bd, lv, wbuf, parts, got, others, ty, out, tz, lsem, wsem, ssem, rsem):
    net = Net(ssem, rsem)
    order = [c * NZ + q for q in range(NZ) for c in range(2)]
    run([exchange_layers(net, part, part_b, tz), gather_dpre(net, d_pre, 1, d_pre_l, bd, lsem.at[0]),
         summed(net, d_pre, w1f, True, dx_out, order, lv, wbuf, parts, got, others, ty, out, lsem.at[1], wsem)], FOURTH_ORDER)
    net.finish()


def comm(body, outs, bufs, n_local, n_remote, *args):
    hbm = pl.BlockSpec(memory_space=pltpu.HBM)
    return pl.pallas_call(
        body,
        out_shape=[jax.ShapeDtypeStruct(s, d) for s, d in outs],
        in_specs=[hbm] * len(args),
        out_specs=[hbm] * len(outs),
        scratch_shapes=[pltpu.VMEM(s, d) for s, d in bufs] + [
            pltpu.SemaphoreType.DMA((n,)) for n in (*n_local, n_remote, n_remote)],
        compiler_params=pltpu.CompilerParams(has_side_effects=True),
        cost_estimate=pl.CostEstimate(flops=80_000_000_000, bytes_accessed=64 << 20, transcendentals=0),
    )(*args)


def solution(mesh):
    act_spec = P(("dep", "row"), "col")
    wgt_spec = P("row", "col")
    grad_spec = P(("row", "dep"), "col")
    bf16, f32 = jnp.bfloat16, jnp.float32
    swap = [(r, r ^ 1) for r in range(2 * NX)]

    def dot(a, b, dims):
        return lax.dot_general(a, b, (dims, ((), ())), preferred_element_type=f32)

    def local_block(x_loc, w_up, w_down, g_loc):
        tb, hb = x_loc.shape
        hr, fb = w_up.shape
        fk = fb // 2
        hid = NY * hb
        tok = 2 * tb
        k = lax.rem(lax.axis_index("row"), 2)

        w1f, w2f, xf, gf, pre_act, act, act_l, g_l = comm(
            first_kernel,
            [((2 * NX * hr, fk), bf16), ((fk, hid), bf16), ((tok, hid), bf16), ((tok, hid), bf16), ((tok, fk), f32), ((tok, fk), bf16),
             ((NX, 4, tok // 4, fk), bf16), ((2 * NX, tb, hb), bf16)],
            [((hr, fk), bf16), ((4, fk // 8, hb), bf16), ((2, fk // 16, hb), bf16), ((2, fk // 16, hb), bf16),
             ((tb, hb), bf16), ((tb, hb), bf16), ((tb, hb), bf16), ((fk // 8, hid), bf16), ((tok, hid), bf16), ((2, hid, fk // 8), bf16),
             ((tok, fk), f32), ((tok, fk), bf16), ((2, 4, tok // 4, fk // 2), bf16), ((2, 2, tok // 8, fk // 2), bf16),
             ((2, 2, tok // 8, fk // 2), bf16)], (9, 2), 160,
            w_up, w_down, x_loc, g_loc)
        d_act = dot(gf, w2f, ((1,), (1,)))
        d_pre = (d_act * gelu_slope(pre_act)).astype(bf16)
        dw_down_part = dot(act_l.reshape(NX * tok, fk), g_l.reshape(NX * tok, hb), ((0,), (0,)))
        dw_down = lax.psum_scatter(dw_down_part, "dep", scatter_dimension=0, tiled=True)

        d_pre, dw_down_part = lax.optimization_barrier((d_pre, dw_down_part))
        sum_bufs = [((4, tok, hb), f32), ((4, tb, hb), f32), ((3, tb, hb), f32), ((2, tb // 2, hb), f32), ((tb, hb), bf16)]
        d_pre_l0, x_l, y_loc = comm(
            third_gather,
            [((NX, tok, fk // 2), bf16), ((2 * NX, tb, hb), bf16), ((tb, hb), bf16)],
            [((tok, fk // 2), bf16), ((tb, hb), bf16), ((2, tb // 2, hb), bf16), ((tok, fk), bf16), ((2, fk, hb // 4), bf16)] + sum_bufs,
            (3, 2), 64,
            d_pre, xf, act, w2f)
        x_l = x_l.reshape(NX * tok, hb)

        def up_part(d_pre_l):
            return dot(x_l, d_pre_l.reshape(NX * tok, fk // 2), ((0,), (0,)))

        part0 = up_part(d_pre_l0)
        part0, dw_down = lax.optimization_barrier((part0, dw_down))
        d_pre_l1, dx_loc, part_b = comm(
            fourth_gather,
            [((NX, tok, fk // 2), bf16), ((tb, hb), bf16), ((3, 2 * hr // NZ, fk // 2), f32)],
            [((tok, fk // 2), bf16), ((tok, fk), bf16), ((2, hb // 4, fk), bf16)] + sum_bufs + [((2, hr // NZ, fk // 2), f32)],
            (2, 2), 40,
            d_pre, w1f, part0)
        own = lax.dynamic_slice_in_dim(part0, lax.axis_index("dep") * (2 * hr // NZ), 2 * hr // NZ, 0)
        totals = [own + part_b[0] + part_b[1] + part_b[2],
                  lax.psum_scatter(up_part(d_pre_l1), "dep", scatter_dimension=0, tiled=True)]
        outs = []
        for total in totals:
            total = total.reshape(2, hr // NZ, fk // 2)
            keep = jnp.where(k == 0, total[0], total[1])
            take = lax.ppermute(jnp.where(k == 0, total[1], total[0]), "row", swap)
            outs.append((jnp.where(k == 0, keep, take), jnp.where(k == 0, take, keep)))
        dw_up = jnp.concatenate([outs[0][0], outs[1][0], outs[0][1], outs[1][1]], axis=1)
        return y_loc, dx_loc, dw_up, dw_down

    return jax.shard_map(local_block, mesh=mesh, in_specs=(act_spec, wgt_spec, wgt_spec, act_spec), out_specs=(act_spec, act_spec, grad_spec, grad_spec), check_vma=False)
```

```python
import jax
import jax.numpy as jnp
from jax import lax
from jax.experimental import pallas as pl
from jax.experimental.pallas import tpu as pltpu
from jax.sharding import PartitionSpec as P

GELU_COEF = 0.7978845608028654
CUBIC_COEF = 0.044715
NX = 4
NY = 4
NZ = 4
FIRST_ORDER = (0, 2, 3, 1, 6, 8, 4, 2, 3, 3, 2, 2, 3, 3, 3, 2, 6, 2, 2, 2, 6, 5, 5, 3, 8, 5, 5, 5, 5, 3, 2, 4, 0, 4, 0, 1, 8, 4, 0, 0, 1, 0, 1, 0, 8, 1, 0, 1, 6, 3, 3, 7, 1, 6, 1, 0, 0, 3, 3, 3, 1, 7, 7, 1, 7, 7, 0, 3, 1)
THIRD_ORDER = (0, 2, 0, 2, 2, 1, 2, 2, 2, 2, 1, 1, 0, 0, 0, 1, 2, 2, 2, 1, 1, 1)
FOURTH_ORDER = (0, 2, 2, 2, 1, 0, 2, 2, 1, 2, 1, 2, 1, 1, 1, 1, 0, 2, 0, 2, 2)


def gelu_fwd(pre_act):
    inner = GELU_COEF * (pre_act + CUBIC_COEF * pre_act * pre_act * pre_act)
    return 0.5 * pre_act * (1.0 + jnp.tanh(inner))


def gelu_slope(pre_act):
    inner = GELU_COEF * (pre_act + CUBIC_COEF * pre_act * pre_act * pre_act)
    tanh_val = jnp.tanh(inner)
    return 0.5 * (1.0 + tanh_val) + 0.5 * pre_act * (1.0 - tanh_val * tanh_val) * GELU_COEF * (1.0 + 3.0 * CUBIC_COEF * pre_act * pre_act)


def rot(v, d, n):
    return lax.rem(v + (d % n), n)


class Net:
    def __init__(self, send_sem, recv_sem):
        self.send_sem, self.recv_sem = send_sem, recv_sem
        self.used = 0
        self.sent = []
        self.z = lax.axis_index("dep")
        self.y = lax.axis_index("col")
        row = lax.axis_index("row")
        self.row = row
        self.x = lax.div(row, 2)
        self.k = lax.rem(row, 2)

    def slots(self, n):
        base = self.used
        self.used += n
        return base

    def make(self, src, dst, where, send_slot, recv_slot):
        return pltpu.make_async_remote_copy(
            src_ref=src, dst_ref=dst, send_sem=self.send_sem.at[send_slot], recv_sem=self.recv_sem.at[recv_slot],
            device_id=where, device_id_type=pl.DeviceIdType.MESH)

    def send(self, src, dst, where):
        slot = self.slots(1)
        copy = self.make(src, dst, where, slot, slot)
        copy.start()
        self.sent.append(copy)
        return copy

    def finish(self):
        for copy in self.sent:
            copy.wait_send()

    def at_x(self, d):
        return {"row": 2 * rot(self.x, d, NX) + self.k}

    def at_y(self, d):
        return {"col": rot(self.y, d, NY)}

    def at_z(self, d):
        return {"dep": rot(self.z, d, NZ)}

    def partner(self):
        return {"row": 2 * self.x + 1 - self.k}


class Gate:
    opened = False


def need(*gates):
    assert all(gate.opened for gate in gates)


def ring(net, place, n, up, down, own, view, arrived, pieces=2):
    west, east, far = rot(place, -1, n), rot(place, 1, n), rot(place, 2, n)
    ups, downs, relays = [], [], []

    def give(q):
        r = pieces - 1 - q
        ups.append(net.send(own(q), view(place, q), up))
        downs.append(net.send(own(r), view(place, r), down))

    give(0)
    give(1)
    for q in range(pieces):
        yield [ups[q], downs[q]]
        r = pieces - 1 - q
        ups[q].wait_recv()
        downs[q].wait_recv()
        if q < pieces // 2:
            relays.append((q, net.send(view(west, q), view(west, q), up)))
            relays.append((r, net.send(view(east, r), view(east, r), down)))
        if q + 2 < pieces:
            give(q + 2)
        arrived(west, q)
        arrived(east, r)
    for n in range(0, len(relays), 2):
        yield [copy for _, copy in relays[n:n + 2]]
        for q, copy in relays[n:n + 2]:
            copy.wait_recv()
            arrived(far, q)


def exchange(net, place, n, up, down, piece, slot, tmp, arrived=lambda j: None):
    west, east, far = rot(place, -1, n), rot(place, 1, n), rot(place, 2, n)
    lo = net.send(piece(far, 0), tmp.at[0], up)
    hi = net.send(piece(far, 1), tmp.at[1], down)
    e = net.send(piece(east, None), slot(place, 0, None), up)
    w = net.send(piece(west, None), slot(place, 1, None), down)
    yield [lo, hi]
    lo.wait_recv()
    lo = net.send(tmp.at[0], slot(west, 2, 0), up)
    hi.wait_recv()
    hi = net.send(tmp.at[1], slot(east, 2, 1), down)
    yield [e, w]
    e.wait_recv()
    arrived(west)
    w.wait_recv()
    arrived(east)
    yield [lo, hi]
    lo.wait_recv()
    hi.wait_recv()
    arrived(far)


def rows_of(base, size, h):
    return pl.ds(base, size) if h is None else pl.ds(base + h * (size // 2), size // 2)


def to_z(net, view, got, pieces):
    def arrived(i, q):
        got.append(net.send(view(i, q), view(i, q), net.at_z(1 if q < pieces // 2 else -1)))
    return arrived


def gather_w1(net, w1, w1f, buf, sem):
    rows, cols = w1.shape[0], w1f.shape[1]
    size = rows // 4
    parity = lax.rem(net.z, 2)
    mine = pl.ds(pl.multiple_of(net.k * cols, cols), cols)
    other = pl.ds(pl.multiple_of((1 - net.k) * cols, cols), cols)

    def slot(i, q, k):
        return w1f.at[pl.ds(pl.multiple_of(i * 8 * size + q * 2 * size + k * size, size), size), :]

    load = pltpu.make_async_copy(w1.at[:, mine], buf, sem)
    load.start()
    swaps = [net.send(w1.at[pl.ds(q * size, size), other], slot(net.x, q, net.k), net.partner()) for q in range(4)]
    yield swaps
    load.wait()
    stores = [pltpu.make_async_copy(buf.at[pl.ds(q * size, size), :], slot(net.x, q, net.k), sem) for q in range(4)]
    for copy in stores:
        copy.start()
    for copy in swaps:
        copy.wait_recv()
    for copy in stores:
        copy.wait()

    def view(i, q):
        return slot(i, q, parity)

    got = []
    yield from ring(net, net.x, NX, net.at_x(1), net.at_x(-1), lambda q: view(net.x, q), view, to_z(net, view, got, 4), 4)
    yield got
    for copy in got:
        copy.wait_recv()


def gather_tokens(net, src, dst, buf, sem, order=None):
    rows, cols = src.shape
    base = pl.multiple_of(net.k * rows, rows)

    def view(j, h):
        return dst.at[rows_of(base, rows, h), pl.ds(pl.multiple_of(j * cols, cols), cols)]

    if order is None:
        loads = [pltpu.make_async_copy(src, buf, sem)]
    else:
        size = cols // len(order)
        loads = [
            pltpu.make_async_copy(src.at[:, pl.ds(b * size, size)], buf.at[:, pl.ds(n * size, size)], sem) for n, b in enumerate(order)]
    for copy in loads:
        copy.start()
    for copy in loads:
        copy.wait()
    src = buf
    passed = [net.send(src, view(net.y, None), net.partner())]

    def arrived(j, h):
        passed.append(net.send(view(j, h), view(j, h), net.partner()))

    gather = ring(net, net.y, NY, net.at_y(1), net.at_y(-1), lambda h: src.at[rows_of(0, rows, h), :], view, arrived)
    first = next(gather)
    store = pltpu.make_async_copy(buf, view(net.y, None), sem)
    store.start()
    yield first
    yield from gather
    yield passed
    store.wait()
    for copy in passed:
        copy.wait_recv()


def move_w2(net, w2, w2s, mid, tx, ty, sem):
    rows, cols = w2.shape
    part = rows // 8
    base = pl.multiple_of(lax.rem(net.z, 2) * 4 * part, part)

    def piece(i, h):
        return w2.at[rows_of(pl.multiple_of(base + i * part, part), part, h), :]

    load = pltpu.make_async_copy(piece(net.x, None), mid.at[net.x], sem)
    load.start()
    yield from exchange(net, net.x, NX, net.at_x(1), net.at_x(-1), piece, lambda j, side, h: mid.at[j, rows_of(0, part, h), :], tx)
    load.wait()

    def slot(j, side, h):
        return w2s.at[rows_of(0, part, h), pl.ds(pl.multiple_of(j * cols, cols), cols)]

    store = pltpu.make_async_copy(mid.at[net.y], slot(net.y, 0, None), sem)
    store.start()
    yield from exchange(net, net.y, NY, net.at_y(1), net.at_y(-1), lambda i, h: mid.at[i, rows_of(0, part, h), :], slot, ty)
    store.wait()


def gather_w2(net, w2s, w2f, sem):
    rows = w2s.shape[0]
    size = rows // 4
    base = lax.rem(net.z, 2) * 4 * rows

    def view(i, q):
        return w2f.at[pl.ds(pl.multiple_of(base + i * rows + q * size, size), size), :]

    def own(q):
        return w2s.at[pl.ds(q * size, size), :]

    got = []
    gather = ring(net, net.x, NX, net.at_x(1), net.at_x(-1), own, view, to_z(net, view, got, 4), 4)
    first = next(gather)
    store = pltpu.make_async_copy(w2s, w2f.at[pl.ds(pl.multiple_of(base + net.x * rows, rows), rows), :], sem)
    store.start()
    yield first
    yield from gather
    yield got
    for copy in got:
        copy.wait_recv()
    store.wait()


def layers_w2(net, w2s, w2f):
    rows = w2s.shape[0]
    size = rows // 4
    base = lax.rem(net.z, 2) * 4 * rows + net.x * rows
    for q in range(2):
        got = []
        for p, d in ((q, 1), (3 - q, -1)):
            got.append(net.send(w2s.at[pl.ds(p * size, size), :], w2f.at[pl.ds(pl.multiple_of(base + p * size, size), size), :], net.at_z(d)))
        yield got
        for copy in got:
            copy.wait_recv()


def move_act(net, act, act_l, cs, mid, tx, ty, sem):
    part = act_l.shape[2]

    def piece(i, h):
        return act.at[rows_of(pl.multiple_of(i * part, part), part, h), cs]

    load = pltpu.make_async_copy(piece(net.y, None), mid.at[net.y], sem)
    load.start()
    yield from exchange(net, net.y, NY, net.at_y(1), net.at_y(-1), piece, lambda j, side, h: mid.at[j, rows_of(0, part, h), :], ty)
    load.wait()
    store = pltpu.make_async_copy(mid.at[net.x], act_l.at[net.x, net.y, :, cs], sem)
    store.start()
    yield from exchange(
        net, net.x, NX, net.at_x(1), net.at_x(-1), lambda i, h: mid.at[i, rows_of(0, part, h), :],
        lambda j, side, h: act_l.at[j, net.y, rows_of(0, part, h), cs], tx)
    store.wait()

    def view(j, h):
        return act_l.at[pl.ds(2 * h, 2), j, :, cs]

    yield from ring(net, net.y, NY, net.at_y(1), net.at_y(-1), lambda h: view(net.y, h), view, lambda i, h: None)


def layer_g(net, g, g_l, buf, sem):
    rows = g.shape[0]
    load = pltpu.make_async_copy(g, buf, sem)
    load.start()

    def view(i, h):
        return g_l.at[2 * i + net.k, rows_of(0, rows, h), :]

    passed = [net.send(g, view(net.x, None), net.partner())]

    def arrived(i, h):
        passed.append(net.send(view(i, h), view(i, h), net.partner()))

    gather = ring(net, net.x, NX, net.at_x(1), net.at_x(-1), lambda h: g.at[rows_of(0, rows, h), :], view, arrived)
    first = next(gather)
    load.wait()
    store = pltpu.make_async_copy(buf, view(net.x, None), sem)
    store.start()
    yield first
    yield from gather
    yield passed
    store.wait()
    for copy in passed:
        copy.wait_recv()


def layer_x(net, xf, x_l, buf, tmp, sem):
    rows, cols = buf.shape
    base = pl.multiple_of(net.k * rows, rows)

    def piece(i, h):
        return xf.at[rows_of(base, rows, h), pl.ds(pl.multiple_of(i * cols, cols), cols)]

    def slot(j, side, h):
        return x_l.at[2 * j + net.k, rows_of(0, rows, h), :]

    load = pltpu.make_async_copy(piece(net.x, None), buf, sem)
    load.start()
    own = slot(net.x, 0, None)
    passed = [net.send(piece(net.x, None), own, net.partner())]

    def arrived(j):
        passed.append(net.send(slot(j, 0, None), slot(j, 0, None), net.partner()))

    moves = exchange(net, net.x, NX, net.at_x(1), net.at_x(-1), piece, slot, tmp, arrived)
    first = next(moves)
    load.wait()
    store = pltpu.make_async_copy(buf, own, sem)
    store.start()
    yield first
    yield from moves
    yield passed
    store.wait()
    for copy in passed:
        copy.wait_recv()


def gather_dpre(net, d_pre, start, d_pre_l, buf, sem):
    rows, cols = buf.shape
    cs = pl.ds(start, cols)
    load = pltpu.make_async_copy(d_pre.at[:, cs], buf, sem)
    load.start()
    size = rows // 4

    def view(i, q):
        return d_pre_l.at[i, pl.ds(q * size, size), :]

    gather = ring(
        net, net.x, NX, net.at_x(1), net.at_x(-1), lambda q: d_pre.at[pl.ds(q * size, size), cs], view, lambda i, q: None, 4)
    first = next(gather)
    load.wait()
    store = pltpu.make_async_copy(buf, d_pre_l.at[net.x], sem)
    store.start()
    yield first
    yield from gather
    store.wait()


def block_tiles(out, lhs, w, base, by_rows, wbuf, wsem):
    size = out.shape[1] // 4

    def fetch(i, slot):
        t = pl.ds(pl.multiple_of(base + i * size, size), size)
        return pltpu.make_async_copy(w.at[t, :] if by_rows else w.at[:, t], wbuf.at[slot], wsem.at[slot])

    fetch(0, 0).start()

    @pl.loop(0, 4)
    def _(i):
        slot = lax.rem(i, 2)

        @pl.when(i < 3)
        def _():
            fetch(i + 1, 1 - slot).start()

        fetch(i, slot).wait()
        dims = (((1,), (1 if by_rows else 0,)), ((), ()))
        out[:, pl.ds(pl.multiple_of(i * size, size), size)] = lax.dot_general(
            lhs[...], wbuf[slot], dims, preferred_element_type=jnp.float32)


def add_own(got, own, k):
    rows = got.shape[0]

    @pl.loop(0, rows, step=16)
    def _(r):
        here = pl.ds(pl.multiple_of(r, 16), 16)
        got[here, :] += own[pl.ds(pl.multiple_of(k * rows + r, 16), 16), :]


def add_all(out, own, others, order):
    rows = out.shape[0]
    size = out.shape[1] // len(order)

    @pl.loop(0, rows, step=16)
    def _(r):
        here = pl.ds(pl.multiple_of(r, 16), 16)
        total = (own[here, :] + others[0, here, :] + others[1, here, :] + others[2, here, :]).astype(out.dtype)
        for n, b in enumerate(order):
            out[here, b * size:(b + 1) * size] = total[:, n * size:(n + 1) * size]


def summed(net, lhs, w, by_rows, dst, order, lv, wbuf, parts, got, others, tmp, out, sem, wsem):
    rows, cols = got.shape[1:]
    load = pltpu.make_async_copy(lhs, lv, sem)
    load.start()
    load.wait()
    other = pl.ds(pl.multiple_of((1 - net.k) * rows, rows), rows)
    up, down = net.at_y(1), net.at_y(-1)
    half = rows // 2
    lower, upper = pl.ds(0, half), pl.ds(half, half)
    swaps = []

    def part(n):
        base = rot(net.y, (2, 1, 3, 0)[n], NY) * cols
        block_tiles(parts.at[n], lv, w, base, by_rows, wbuf, wsem)
        swaps.append(net.send(parts.at[n, other], got.at[n], net.partner()))

    def add(n):
        swaps[n].wait_recv()
        add_own(got.at[n], parts.at[n], net.k)

    part(0)
    yield []
    part(1)
    yield [swaps[0]]
    add(0)
    part(2)
    lo = net.send(got.at[0, lower], tmp.at[0], up)
    hi = net.send(got.at[0, upper], tmp.at[1], down)
    yield [swaps[1]]
    add(1)
    part(3)
    e = net.send(got.at[1], others.at[0], up)
    yield [swaps[2]]
    add(2)
    yield [swaps[3]]
    add(3)
    w_ = net.send(got.at[2], others.at[1], down)
    yield [lo, hi]
    lo.wait_recv()
    lo = net.send(tmp.at[0], others.at[2, lower], up)
    hi.wait_recv()
    hi = net.send(tmp.at[1], others.at[2, upper], down)
    yield [e, w_]
    e.wait_recv()
    w_.wait_recv()
    yield [lo, hi]
    lo.wait_recv()
    hi.wait_recv()
    add_all(out, got.at[3], others, order)
    store = pltpu.make_async_copy(out, dst, sem)
    store.start()
    yield []
    store.wait()


def exchange_layers(net, part, dst, tmp):
    rows = dst.shape[1]

    def piece(i, h):
        return part.at[rows_of(pl.multiple_of(i * rows, rows), rows, h), :]

    yield from exchange(
        net, net.z, NZ, net.at_z(1), net.at_z(-1), piece, lambda j, side, h: dst.at[side, rows_of(0, rows, h), :], tmp)


def run(flows, order=()):
    for n in order:
        next(flows[n], None)
    flows = list(flows)
    while flows:
        flows = [f for f in flows if next(f, flows) is not flows]


def up_tiles(first, w1f, xv, wbuf, uv, av, wsem):
    cols = wbuf.shape[2]

    def fetch(i, slot):
        t = pl.ds(pl.multiple_of((first + i) * cols, cols), cols)
        return pltpu.make_async_copy(w1f.at[:, t], wbuf.at[slot], wsem.at[slot])

    fetch(0, 0).start()

    @pl.loop(0, 4)
    def _(i):
        slot = lax.rem(i, 2)

        @pl.when(i < 3)
        def _():
            fetch(i + 1, 1 - slot).start()

        fetch(i, slot).wait()
        t = pl.ds(pl.multiple_of((first + i) * cols, cols), cols)
        u = jnp.dot(xv[...], wbuf[slot], preferred_element_type=jnp.float32)
        uv[:, t] = u
        av[:, t] = gelu_fwd(u).astype(av.dtype)


def first_kernel(
        w1, w2, x, g, w1f, w2f, xf, gf, pre, act, act_l, g_l, b1, mid, tx, ty, bx, bg, bl, w2s, xv, wbuf, uv, av, mids, txa, tya,
        lsem, wsem, ssem, rsem):
    net = Net(ssem, rsem)
    cols = act.shape[1] // 2
    chunks = [pl.ds(c * cols, cols) for c in range(2)]
    w1_here, x_here, a_here, w2_moved = Gate(), Gate(), [Gate(), Gate()], Gate()

    def weights1():
        yield from gather_w1(net, w1, w1f, b1, lsem.at[0])
        w1_here.opened = True

    def tokens_x():
        yield from gather_tokens(net, x, xf, bx, lsem.at[1], [c * NZ + q for q in range(NZ) for c in range(2)])
        fetch = pltpu.make_async_copy(xf, xv, lsem.at[1])
        fetch.start()
        yield []
        fetch.wait()
        x_here.opened = True

    def weights2():
        yield from move_w2(net, w2, w2s, mid, tx, ty, lsem.at[3])
        w2_moved.opened = True
        yield from gather_w2(net, w2s, w2f, lsem.at[3])

    def up():
        yield [w1_here, x_here]
        need(w1_here, x_here)
        for c in range(2):
            up_tiles(4 * c, w1f, xv, wbuf, uv, av, wsem)
            keep_a = pltpu.make_async_copy(av.at[:, chunks[c]], act.at[:, chunks[c]], lsem.at[6])
            keep_u = pltpu.make_async_copy(uv.at[:, chunks[c]], pre.at[:, chunks[c]], lsem.at[7])
            keep_a.start()
            keep_u.start()
            keep_a.wait()
            keep_u.wait()
            a_here[c].opened = True
            yield []

    def acts(c):
        yield [a_here[c]]
        need(a_here[c])
        yield from move_act(net, act, act_l, chunks[c], mids.at[c], txa.at[c], tya.at[c], lsem.at[4 + c])

    def weights2_own():
        yield [w2_moved]
        need(w2_moved)
        yield from layers_w2(net, w2s, w2f)

    def layer():
        yield from layer_g(net, g, g_l, bl, lsem.at[8])

    flows = [acts(0), acts(1), weights1(), weights2(), up(), tokens_x(), gather_tokens(net, g, gf, bg, lsem.at[2]), layer(), weights2_own()]
    run(flows, FIRST_ORDER)
    net.finish()


def third_gather(
        d_pre, xf, act, w2f, d_pre_l, x_l, y_out, bd, bx, tx, lv, wbuf, parts, got, others, ty, out, lsem, wsem, ssem, rsem):
    net = Net(ssem, rsem)
    run([layer_x(net, xf, x_l, bx, tx, lsem.at[1]), gather_dpre(net, d_pre, 0, d_pre_l, bd, lsem.at[0]),
         summed(net, act, w2f, False, y_out, [0], lv, wbuf, parts, got, others, ty, out, lsem.at[2], wsem)], THIRD_ORDER)
    net.finish()


def fourth_gather(
        d_pre, w1f, part, d_pre_l, dx_out, part_b, bd, lv, wbuf, parts, got, others, ty, out, tz, lsem, wsem, ssem, rsem):
    net = Net(ssem, rsem)
    order = [c * NZ + q for q in range(NZ) for c in range(2)]
    run([exchange_layers(net, part, part_b, tz), gather_dpre(net, d_pre, d_pre.shape[1] - bd.shape[1], d_pre_l, bd, lsem.at[0]),
         summed(net, d_pre, w1f, True, dx_out, order, lv, wbuf, parts, got, others, ty, out, lsem.at[1], wsem)], FOURTH_ORDER)
    net.finish()


def comm(body, outs, bufs, n_local, n_remote, *args):
    hbm = pl.BlockSpec(memory_space=pltpu.HBM)
    return pl.pallas_call(
        body,
        out_shape=[jax.ShapeDtypeStruct(s, d) for s, d in outs],
        in_specs=[hbm] * len(args),
        out_specs=[hbm] * len(outs),
        scratch_shapes=[pltpu.VMEM(s, d) for s, d in bufs] + [
            pltpu.SemaphoreType.DMA((n,)) for n in (*n_local, n_remote, n_remote)],
        compiler_params=pltpu.CompilerParams(has_side_effects=True),
        cost_estimate=pl.CostEstimate(flops=80_000_000_000, bytes_accessed=64 << 20, transcendentals=0),
    )(*args)


def solution(mesh):
    act_spec = P(("dep", "row"), "col")
    wgt_spec = P("row", "col")
    grad_spec = P(("row", "dep"), "col")
    bf16, f32 = jnp.bfloat16, jnp.float32
    swap = [(r, r ^ 1) for r in range(2 * NX)]

    def dot(a, b, dims):
        return lax.dot_general(a, b, (dims, ((), ())), preferred_element_type=f32)

    def local_block(x_loc, w_up, w_down, g_loc):
        tb, hb = x_loc.shape
        hr, fb = w_up.shape
        fk = fb // 2
        hid = NY * hb
        tok = 2 * tb
        k = lax.rem(lax.axis_index("row"), 2)

        w1f, w2f, xf, gf, pre_act, act, act_l, g_l = comm(
            first_kernel,
            [((2 * NX * hr, fk), bf16), ((fk, hid), bf16), ((tok, hid), bf16), ((tok, hid), bf16), ((tok, fk), f32), ((tok, fk), bf16),
             ((NX, 4, tok // 4, fk), bf16), ((2 * NX, tb, hb), bf16)],
            [((hr, fk), bf16), ((4, fk // 8, hb), bf16), ((2, fk // 16, hb), bf16), ((2, fk // 16, hb), bf16),
             ((tb, hb), bf16), ((tb, hb), bf16), ((tb, hb), bf16), ((fk // 8, hid), bf16), ((tok, hid), bf16), ((2, hid, fk // 8), bf16),
             ((tok, fk), f32), ((tok, fk), bf16), ((2, 4, tok // 4, fk // 2), bf16), ((2, 2, tok // 8, fk // 2), bf16),
             ((2, 2, tok // 8, fk // 2), bf16)], (9, 2), 160,
            w_up, w_down, x_loc, g_loc)
        d_act = dot(gf, w2f, ((1,), (1,)))
        d_pre = (d_act * gelu_slope(pre_act)).astype(bf16)
        dw_down_part = dot(act_l.reshape(NX * tok, fk), g_l.reshape(NX * tok, hb), ((0,), (0,)))
        dw_down = lax.psum_scatter(dw_down_part, "dep", scatter_dimension=0, tiled=True)

        d_pre, dw_down_part = lax.optimization_barrier((d_pre, dw_down_part))
        sum_bufs = [((4, tok, hb), f32), ((4, tb, hb), f32), ((3, tb, hb), f32), ((2, tb // 2, hb), f32), ((tb, hb), bf16)]
        f0 = fk * 5 // 8
        f1 = fk - f0
        d_pre_l0, x_l, y_loc = comm(
            third_gather,
            [((NX, tok, f0), bf16), ((2 * NX, tb, hb), bf16), ((tb, hb), bf16)],
            [((tok, f0), bf16), ((tb, hb), bf16), ((2, tb // 2, hb), bf16), ((tok, fk), bf16), ((2, fk, hb // 4), bf16)] + sum_bufs,
            (3, 2), 64,
            d_pre, xf, act, w2f)
        x_l = x_l.reshape(NX * tok, hb)

        def up_part(d_pre_l):
            return dot(x_l, d_pre_l.reshape(NX * tok, -1), ((0,), (0,)))

        part0 = up_part(d_pre_l0)
        part0, dw_down = lax.optimization_barrier((part0, dw_down))
        d_pre_l1, dx_loc, part_b = comm(
            fourth_gather,
            [((NX, tok, f1), bf16), ((tb, hb), bf16), ((3, 2 * hr // NZ, f0), f32)],
            [((tok, f1), bf16), ((tok, fk), bf16), ((2, hb // 4, fk), bf16)] + sum_bufs + [((2, hr // NZ, f0), f32)],
            (2, 2), 40,
            d_pre, w1f, part0)
        own = lax.dynamic_slice_in_dim(part0, lax.axis_index("dep") * (2 * hr // NZ), 2 * hr // NZ, 0)
        totals = [own + part_b[0] + part_b[1] + part_b[2],
                  lax.psum_scatter(up_part(d_pre_l1), "dep", scatter_dimension=0, tiled=True)]
        outs = []
        for total in totals:
            total = total.reshape(2, hr // NZ, -1)
            keep = jnp.where(k == 0, total[0], total[1])
            take = lax.ppermute(jnp.where(k == 0, total[1], total[0]), "row", swap)
            outs.append((jnp.where(k == 0, keep, take), jnp.where(k == 0, take, keep)))
        dw_up = jnp.concatenate([outs[0][0], outs[1][0], outs[0][1], outs[1][1]], axis=1)
        return y_loc, dx_loc, dw_up, dw_down

    return jax.shard_map(local_block, mesh=mesh, in_specs=(act_spec, wgt_spec, wgt_spec, act_spec), out_specs=(act_spec, act_spec, grad_spec, grad_spec), check_vma=False)
```
